32 devices in a mesh: gx: 4 (over x, core), gy: 4 (over z), gz: 2 (over y).
Axes of the slice: x: 2, y: 2, z: 4, core: 2. Of those that a mesh axis runs over, the one named last changes fastest.
Arguments:
- kappa: float32 [5, 5, 5, 4, 4, 128], P(None, None, None, 'gx', 'gy', 'gz'), may hold values from 0.2 to 5
- source: float32 [5, 5, 5, 4, 4, 128], P(None, None, None, 'gx', 'gy', 'gz'), may hold values from -24 to 24
Outputs:
- solution: float32 [16, 16, 512], P('gx', 'gy', 'gz')
- residual: float32 [16, 16, 512], P('gx', 'gy', 'gz')
The draws below stay inside these ranges and needn't reach their ends.
All inputs are finite; a program needn't handle non-finite values.
Results may differ from the reference program's by a relative error of at most 0.0003.
Values sent between devices are 32-bit elements; how exact they have to be, the bound alone decides.
A program may use at most 64 MiB of HBM per device.

```python
import math
import jax
import jax.numpy as jnp
import numpy as np
from jax import lax

POLY_DEGREE = 4
LEVELS = 3
SWEEPS = 2
ELEMENTS_X = 4
ELEMENTS_Y = 4
ELEMENTS_Z = 128


def level_of(own_key, shape, pieces, smallest, top_value):
    def one(position, blocks):
        steps = jax.random.uniform(jax.random.fold_in(jax.random.fold_in(own_key, 6), position), (blocks,), jnp.float32, smallest / len(pieces), top_value / len(pieces))
        return jnp.repeat(jnp.exp(steps), shape[position] // blocks).reshape((-1,) + (1,) * (len(shape) - position - 1))

    gain = one(*pieces[0])
    for cut in pieces[1:]:
        gain = gain * one(*cut)
    return gain


def bell_draw(own_key, dims, scale, reach, cuts=(), kind=jnp.bfloat16):
    result = jax.random.normal(own_key, dims, jnp.float32) * scale
    if len(cuts) > 0:
        result = level_of(own_key, dims, cuts, -0.22, 0.18) * result
    return jnp.clip(result, min=-reach, max=reach).astype(kind)


def setup_inputs(seed: int = 0) -> dict:
    splits = jax.random.split(jax.random.key(seed), 3)
    kappa = jnp.clip(jnp.exp(math.log(5.0) - 3.218876 * jax.random.uniform(splits[0], (POLY_DEGREE + 1, POLY_DEGREE + 1, POLY_DEGREE + 1, ELEMENTS_X, ELEMENTS_Y, ELEMENTS_Z), jnp.float32) ** level_of(splits[0], (POLY_DEGREE + 1, POLY_DEGREE + 1, POLY_DEGREE + 1, ELEMENTS_X, ELEMENTS_Y, ELEMENTS_Z), ((3, 4), (4, 4), (5, 2)), -0.2, 0.2)), 0.2, 5.0)
    source = bell_draw(splits[1], (POLY_DEGREE + 1, POLY_DEGREE + 1, POLY_DEGREE + 1, ELEMENTS_X, ELEMENTS_Y, ELEMENTS_Z), 4.0, 24.0, ((3, 4), (4, 4), (5, 2)), jnp.float32)
    return dict(kappa=kappa, source=source)


relax_weight = 0.6

def gll_tables():
    points = np.array([-1.0, -math.sqrt(3.0 / 7.0), 0.0, math.sqrt(3.0 / 7.0), 1.0])
    quad_weights = np.array([0.1, 49.0 / 90.0, 32.0 / 45.0, 49.0 / 90.0, 0.1])
    bary = np.array([np.prod([points[i] - points[k] for k in range(5) if k != i]) for i in range(5)])
    deriv = np.zeros((5, 5))
    for i in range(5):
        for j in range(5):
            if i != j:
                deriv[i, j] = bary[i] / (bary[j] * (points[i] - points[j]))
    for i in range(5):
        deriv[i, i] = -np.sum(deriv[i])
    return (jnp.asarray(points, jnp.float32), jnp.asarray(quad_weights, jnp.float32), jnp.asarray(deriv, jnp.float32))

def split_first(values):
    count = (values.shape[0] - 1) // 4
    lower = jnp.swapaxes(values[:-1].reshape((count, 4) + values.shape[1:]), 0, 1)
    return jnp.concatenate([lower, values[4::4][None]], axis=0)

def merge_first(block):
    count = block.shape[1]
    rest = block.shape[2:]
    lower = jnp.swapaxes(block[:4], 0, 1).reshape((4 * count,) + rest)
    tail = jnp.concatenate([jnp.zeros((count, 3) + rest, block.dtype), block[4][:, None]], axis=1)
    tail = tail.reshape((4 * count,) + rest)
    spare = [(0, 0)] * len(rest)
    return jnp.pad(lower, [(0, 1)] + spare) + jnp.pad(tail, [(1, 0)] + spare)

def element_view(field):
    element_portion = split_first(field)
    element_portion = split_first(jnp.moveaxis(element_portion, 2, 0))
    element_portion = split_first(jnp.moveaxis(element_portion, 4, 0))
    return jnp.transpose(element_portion, (4, 2, 0, 5, 3, 1))

def node_sum(block):
    element_portion = jnp.transpose(block, (2, 5, 1, 4, 0, 3))
    element_portion = jnp.moveaxis(merge_first(element_portion), 0, 4)
    element_portion = jnp.moveaxis(merge_first(element_portion), 0, 2)
    return merge_first(element_portion)

def stiffness_terms(field, weighted, deriv):
    highest = lax.Precision.HIGHEST
    local = element_view(field)
    grad_x = jnp.einsum('ia,abcxyz->ibcxyz', deriv, local, precision=highest)
    grad_y = jnp.einsum('jb,abcxyz->ajcxyz', deriv, local, precision=highest)
    grad_z = jnp.einsum('kc,abcxyz->abkxyz', deriv, local, precision=highest)
    back = jnp.einsum('ia,ibcxyz->abcxyz', deriv, weighted * grad_x, precision=highest)
    back = back + jnp.einsum('jb,ajcxyz->abcxyz', deriv, weighted * grad_y, precision=highest)
    back = back + jnp.einsum('kc,abkxyz->abcxyz', deriv, weighted * grad_z, precision=highest)
    return node_sum(back)

def mass_pair(paired, width):
    return jnp.stack([width / 6.0 * (2.0 * paired[0] + paired[1]), width / 6.0 * (paired[0] + 2.0 * paired[1])])

def stiff_pair(paired, width):
    slope = (paired[0] - paired[1]) / width
    return jnp.stack([slope, -slope])

def lor_terms(field, coeff, spacing):
    width_x, width_y, width_z = spacing
    zpairs = jnp.stack([field[:, :, :-1], field[:, :, 1:]])
    zmass = mass_pair(zpairs, width_z)
    stiffness_along_z = stiff_pair(zpairs, width_z)
    ymass = jnp.stack([zmass[:, :, :-1], zmass[:, :, 1:]])
    ystiff = jnp.stack([stiffness_along_z[:, :, :-1], stiffness_along_z[:, :, 1:]])
    column_y = width_y[:, None]
    first = mass_pair(ymass, column_y)
    second = stiff_pair(ymass, column_y) + mass_pair(ystiff, column_y)
    column_x = width_x[:, None, None]
    xfirst = jnp.stack([first[:, :, :-1], first[:, :, 1:]])
    xsecond = jnp.stack([second[:, :, :-1], second[:, :, 1:]])
    cells = (stiff_pair(xfirst, column_x) + mass_pair(xsecond, column_x)) * coeff
    total = jnp.zeros(field.shape, jnp.float32)
    for a in range(2):
        for b in range(2):
            for c in range(2):
                total = total + jnp.pad(cells[a, b, c], ((a, 1 - a), (b, 1 - b), (c, 1 - c)))
    return total

def lor_diagonal(coeff, spacing):
    width_x = spacing[0][:, None, None]
    width_y = spacing[1][None, :, None]
    width_z = spacing[2][None, None, :]
    cells = coeff * (width_y * width_z / (9.0 * width_x) + width_x * width_z / (9.0 * width_y) + width_x * width_y / (9.0 * width_z))
    shape = tuple((n + 1 for n in coeff.shape))
    total = jnp.zeros(shape, jnp.float32)
    for a in range(2):
        for b in range(2):
            for c in range(2):
                total = total + jnp.pad(cells, ((a, 1 - a), (b, 1 - b), (c, 1 - c)))
    return total

def subcell_coefficient(kappa):
    averaged = 0.5 * (kappa[:-1] + kappa[1:])
    averaged = 0.5 * (averaged[:, :-1] + averaged[:, 1:])
    averaged = 0.5 * (averaged[:, :, :-1] + averaged[:, :, 1:])
    count_x, count_y, count_z = averaged.shape[3:]
    return jnp.transpose(averaged, (3, 0, 4, 1, 5, 2)).reshape(4 * count_x, 4 * count_y, 4 * count_z)

def coarsen(coeff):
    nx, ny, nz = coeff.shape
    return lax.optimization_barrier(jnp.mean(coeff.reshape(nx // 2, 2, ny // 2, 2, nz // 2, 2), axis=(1, 3, 5)))

def interp_weights(width):
    paired = width.reshape(-1, 2)
    span = paired[:, 0] + paired[:, 1]
    return (paired[:, 1] / span, paired[:, 0] / span)

def prolong_first(coarse, left, right):
    shape = (-1,) + (1,) * (coarse.ndim - 1)
    middle = left.reshape(shape) * coarse[:-1] + right.reshape(shape) * coarse[1:]
    woven = jnp.stack([coarse[:-1], middle], axis=1).reshape((2 * (coarse.shape[0] - 1),) + coarse.shape[1:])
    return jnp.concatenate([woven, coarse[-1:]], axis=0)

def restrict_first(fine, left, right):
    shape = (-1,) + (1,) * (fine.ndim - 1)
    middle = fine[1::2]
    spare = [(0, 0)] * (fine.ndim - 1)
    return fine[0::2] + jnp.pad(left.reshape(shape) * middle, [(0, 1)] + spare) + jnp.pad(right.reshape(shape) * middle, [(1, 0)] + spare)

def prolong(coarse, weight_sets):
    for axis in range(3):
        left, right = weight_sets[axis]
        coarse = jnp.moveaxis(prolong_first(jnp.moveaxis(coarse, axis, 0), left, right), 0, axis)
    return coarse

def restrict(fine, weight_sets):
    for axis in range(3):
        left, right = weight_sets[axis]
        fine = jnp.moveaxis(restrict_first(jnp.moveaxis(fine, axis, 0), left, right), 0, axis)
    return fine

def edge_mask(shape):
    masks = []
    for n in shape:
        index = jnp.arange(n + 1)
        masks.append(((index > 0) & (index < n)).astype(jnp.float32))
    return masks[0][:, None, None] * masks[1][None, :, None] * masks[2][None, None, :]

def cycle(level, forcing, levels):
    coeff, spacing, diag, mask, weight_sets = levels[level]
    guess = relax_weight * forcing / diag
    if level == LEVELS - 1:
        for sweep in range(SWEEPS - 1):
            guess = guess + relax_weight * (forcing - mask * lor_terms(guess, coeff, spacing)) / diag
        return guess
    defect = forcing - lor_terms(guess, coeff, spacing)
    coarse = levels[level + 1][3] * restrict(defect, weight_sets)
    guess = guess + prolong(cycle(level + 1, coarse, levels), weight_sets)
    return guess + relax_weight * (forcing - mask * lor_terms(guess, coeff, spacing)) / diag

def reference(kappa, source):
    points, quad_weights, deriv = gll_tables()
    cube = (quad_weights[:, None, None] * quad_weights[None, :, None] * quad_weights[None, None, :]).reshape(5, 5, 5, 1, 1, 1)
    weighted = kappa * cube
    counts = kappa.shape[3:]
    finest_mask = edge_mask([4 * c for c in counts])
    rhs = finest_mask * node_sum(cube * source)
    gaps = points[1:] - points[:-1]
    spacing = [jnp.tile(gaps, c) for c in counts]
    coeff = subcell_coefficient(kappa)
    levels = []
    for level in range(LEVELS):
        weight_sets = [interp_weights(h) for h in spacing] if level < LEVELS - 1 else None
        levels.append((coeff, spacing, lor_diagonal(coeff, spacing), edge_mask(coeff.shape), weight_sets))
        if level < LEVELS - 1:
            coeff = coarsen(coeff)
            spacing = [h.reshape(-1, 2).sum(axis=1) for h in spacing]

    def operator(field):
        return finest_mask * stiffness_terms(field, weighted, deriv)
    resid = rhs
    precond = cycle(0, resid, levels)
    rho_old = jnp.sum(resid * precond)
    direction = precond
    image = operator(direction)
    alpha = rho_old / jnp.sum(direction * image)
    iterate = alpha * direction
    resid = resid - alpha * image
    precond = cycle(0, resid, levels)
    rho_new = jnp.sum(resid * precond)
    direction = precond + rho_new / rho_old * direction
    image = operator(direction)
    alpha = rho_new / jnp.sum(direction * image)
    iterate = iterate + alpha * direction
    resid = resid - alpha * image
    return (iterate[1:, 1:, 1:], resid[1:, 1:, 1:])
```

```python
import math

import jax
import jax.numpy as jnp
import numpy as np
from jax import lax
from jax.experimental import pallas as pl
from jax.experimental.pallas import tpu as pltpu
from jax.sharding import PartitionSpec as P

LEVELS = 3


relax_weight = 0.6


def extended(cells, sides, width):
    for axis, dim in sides:
        count = lax.axis_size(axis)
        ends = count - 1
        head = lax.slice_in_dim(cells, 0, width, axis=dim)
        tail = lax.slice_in_dim(cells, cells.shape[dim] - width, cells.shape[dim], axis=dim)
        cells = jnp.concatenate(
            [
                lax.ppermute(tail, axis, [(i, (i + 1) % count) for i in range(ends)]),
                cells,
                lax.ppermute(head, axis, [((i + 1) % count, i) for i in range(ends)]),
            ],
            axis=dim,
        )
    return cells


def gll_tables():
    points = np.array([-1.0, -math.sqrt(3.0 / 7.0), 0.0, math.sqrt(3.0 / 7.0), 1.0])
    quad_weights = np.array([0.1, 49.0 / 90.0, 32.0 / 45.0, 49.0 / 90.0, 0.1])
    bary = np.array(
        [np.prod([points[i] - points[k] for k in range(5) if k != i]) for i in range(5)]
    )
    deriv = np.zeros((5, 5))
    for i in range(5):
        for j in range(5):
            if i != j:
                deriv[i, j] = bary[i] / (bary[j] * (points[i] - points[j]))
    for i in range(5):
        deriv[i, i] = -np.sum(deriv[i])
    return (
        jnp.asarray(points, jnp.float32),
        jnp.asarray(quad_weights, jnp.float32),
        jnp.asarray(deriv, jnp.float32),
    )


def split_first(values):
    count = (values.shape[0] - 1) // 4
    lower = jnp.swapaxes(values[:-1].reshape((count, 4) + values.shape[1:]), 0, 1)
    return jnp.concatenate([lower, values[4::4][None]], axis=0)


def merge_first(block):
    count = block.shape[1]
    rest = block.shape[2:]
    lower = jnp.swapaxes(block[:4], 0, 1).reshape((4 * count,) + rest)
    tail = jnp.concatenate([jnp.zeros((count, 3) + rest, block.dtype), block[4][:, None]], axis=1)
    tail = tail.reshape((4 * count,) + rest)
    spare = [(0, 0)] * len(rest)
    return jnp.pad(lower, [(0, 1)] + spare) + jnp.pad(tail, [(1, 0)] + spare)


def element_view(field):
    element_portion = split_first(field)
    element_portion = split_first(jnp.moveaxis(element_portion, 2, 0))
    element_portion = split_first(jnp.moveaxis(element_portion, 4, 0))
    return jnp.transpose(element_portion, (4, 2, 0, 5, 3, 1))


def node_sum(block):
    element_portion = jnp.transpose(block, (2, 5, 1, 4, 0, 3))
    element_portion = jnp.moveaxis(merge_first(element_portion), 0, 4)
    element_portion = jnp.moveaxis(merge_first(element_portion), 0, 2)
    return merge_first(element_portion)


def stiffness_terms(field, weighted, deriv):
    highest = lax.Precision.HIGHEST
    local = element_view(field)
    grad_x = jnp.einsum("ia,abcxyz->ibcxyz", deriv, local, precision=highest)
    grad_y = jnp.einsum("jb,abcxyz->ajcxyz", deriv, local, precision=highest)
    grad_z = jnp.einsum("kc,abcxyz->abkxyz", deriv, local, precision=highest)
    back = jnp.einsum("ia,ibcxyz->abcxyz", deriv, weighted * grad_x, precision=highest)
    back = back + jnp.einsum("jb,ajcxyz->abcxyz", deriv, weighted * grad_y, precision=highest)
    back = back + jnp.einsum("kc,abkxyz->abcxyz", deriv, weighted * grad_z, precision=highest)
    return node_sum(back)


def mass_pair(paired, width):
    return jnp.stack(
        [width / 6.0 * (2.0 * paired[0] + paired[1]), width / 6.0 * (paired[0] + 2.0 * paired[1])]
    )


def stiff_pair(paired, width):
    slope = (paired[0] - paired[1]) / width
    return jnp.stack([slope, -slope])


def lor_terms(field, coeff, spacing):
    width_x, width_y, width_z = spacing
    zpairs = jnp.stack([field[:, :, :-1], field[:, :, 1:]])
    zmass = mass_pair(zpairs, width_z)
    stiffness_along_z = stiff_pair(zpairs, width_z)
    ymass = jnp.stack([zmass[:, :, :-1], zmass[:, :, 1:]])
    ystiff = jnp.stack([stiffness_along_z[:, :, :-1], stiffness_along_z[:, :, 1:]])
    column_y = width_y[:, None]
    first = mass_pair(ymass, column_y)
    second = stiff_pair(ymass, column_y) + mass_pair(ystiff, column_y)
    column_x = width_x[:, None, None]
    xfirst = jnp.stack([first[:, :, :-1], first[:, :, 1:]])
    xsecond = jnp.stack([second[:, :, :-1], second[:, :, 1:]])
    cells = (stiff_pair(xfirst, column_x) + mass_pair(xsecond, column_x)) * coeff
    total = jnp.zeros(field.shape, jnp.float32)
    for a in range(2):
        for b in range(2):
            for c in range(2):
                total = total + jnp.pad(cells[a, b, c], ((a, 1 - a), (b, 1 - b), (c, 1 - c)))
    return total


def lor_diagonal(coeff, spacing):
    width_x = spacing[0][:, None, None]
    width_y = spacing[1][None, :, None]
    width_z = spacing[2][None, None, :]
    cells = coeff * (
        width_y * width_z / (9.0 * width_x)
        + width_x * width_z / (9.0 * width_y)
        + width_x * width_y / (9.0 * width_z)
    )
    shape = tuple((n + 1 for n in coeff.shape))
    total = jnp.zeros(shape, jnp.float32)
    for a in range(2):
        for b in range(2):
            for c in range(2):
                total = total + jnp.pad(cells, ((a, 1 - a), (b, 1 - b), (c, 1 - c)))
    return total


def subcell_coefficient(kappa):
    averaged = 0.5 * (kappa[:-1] + kappa[1:])
    averaged = 0.5 * (averaged[:, :-1] + averaged[:, 1:])
    averaged = 0.5 * (averaged[:, :, :-1] + averaged[:, :, 1:])
    count_x, count_y, count_z = averaged.shape[3:]
    return jnp.transpose(averaged, (3, 0, 4, 1, 5, 2)).reshape(
        4 * count_x, 4 * count_y, 4 * count_z
    )


def coarsen(coeff):
    nx, ny, nz = coeff.shape
    return jnp.mean(coeff.reshape(nx // 2, 2, ny // 2, 2, nz // 2, 2), axis=(1, 3, 5))


def interp_weights(width):
    paired = width.reshape(-1, 2)
    span = paired[:, 0] + paired[:, 1]
    return (paired[:, 1] / span, paired[:, 0] / span)


def prolong_first(coarse, left, right):
    shape = (-1,) + (1,) * (coarse.ndim - 1)
    middle = left.reshape(shape) * coarse[:-1] + right.reshape(shape) * coarse[1:]
    woven = jnp.stack([coarse[:-1], middle], axis=1).reshape(
        (2 * (coarse.shape[0] - 1),) + coarse.shape[1:]
    )
    return jnp.concatenate([woven, coarse[-1:]], axis=0)


def restrict_first(fine, left, right):
    shape = (-1,) + (1,) * (fine.ndim - 1)
    middle = fine[1::2]
    spare = [(0, 0)] * (fine.ndim - 1)
    return (
        fine[0::2]
        + jnp.pad(left.reshape(shape) * middle, [(0, 1)] + spare)
        + jnp.pad(right.reshape(shape) * middle, [(1, 0)] + spare)
    )


def prolong(coarse, weight_sets):
    for axis in range(3):
        left, right = weight_sets[axis]
        coarse = jnp.moveaxis(prolong_first(jnp.moveaxis(coarse, axis, 0), left, right), 0, axis)
    return coarse


def restrict(fine, weight_sets):
    for axis in range(3):
        left, right = weight_sets[axis]
        fine = jnp.moveaxis(restrict_first(jnp.moveaxis(fine, axis, 0), left, right), 0, axis)
    return fine


def collapse_leading(padded):
    inner = padded[1:-1]
    head = inner[0] + padded[0]
    tail = inner[-1] + padded[-1]
    return jnp.concatenate([head[None], inner[1:-1], tail[None]], axis=0)


def fold_axis(padded, axis):
    return jnp.moveaxis(collapse_leading(jnp.moveaxis(padded, axis, 0)), 0, axis)


def assemble(partial_value):
    padded = extended(partial_value, (("gx", 0), ("gy", 1), ("gz", 2)), 1)
    return fold_axis(fold_axis(fold_axis(padded, 0), 1), 2)


def side_mask(cells, position, devices):
    index = position * cells + jnp.arange(cells + 1)
    return ((index > 0) & (index < cells * devices)).astype(jnp.float32)


def block_mask(shape):
    mask_x = side_mask(shape[0], lax.axis_index("gx"), lax.axis_size("gx"))
    mask_y = side_mask(shape[1], lax.axis_index("gy"), lax.axis_size("gy"))
    mask_z = side_mask(shape[2], lax.axis_index("gz"), lax.axis_size("gz"))
    return mask_x[:, None, None] * mask_y[None, :, None] * mask_z[None, None, :]


def owned_mask(shape):
    sides = [(jnp.arange(n + 1) >= 1).astype(jnp.float32) for n in shape]
    return sides[0][:, None, None] * sides[1][None, :, None] * sides[2][None, None, :]


def cycle(level, forcing, levels):
    coeff, spacing, diag, mask, weight_sets, owned = levels[level]
    guess = relax_weight * forcing / diag
    if level == LEVELS - 1:
        guess = (
            guess
            + relax_weight * (forcing - mask * assemble(lor_terms(guess, coeff, spacing))) / diag
        )
        return guess
    defect = forcing * owned - lor_terms(guess, coeff, spacing)
    coarse = levels[level + 1][3] * assemble(restrict(defect, weight_sets))
    guess = guess + prolong(cycle(level + 1, coarse, levels), weight_sets)
    return (
        guess + relax_weight * (forcing - mask * assemble(lor_terms(guess, coeff, spacing))) / diag
    )


def inner_pair(resid, precond, image):
    local_rho = jnp.sum(resid[1:, 1:, 1:] * precond[1:, 1:, 1:])
    local_curv = jnp.sum(precond[1:, 1:, 1:] * image[1:, 1:, 1:])
    return lax.psum((local_rho, local_curv), ("gx", "gy", "gz"))


def distributed_body(kappa, source):
    points, quad_weights, deriv = gll_tables()
    cube = (
        quad_weights[:, None, None] * quad_weights[None, :, None] * quad_weights[None, None, :]
    ).reshape(5, 5, 5, 1, 1, 1)
    weighted = kappa * cube
    counts = kappa.shape[3:]
    finest_mask = block_mask([4 * c for c in counts])
    rhs = finest_mask * assemble(node_sum(cube * source))
    gaps = points[1:] - points[:-1]
    spacing = [jnp.tile(gaps, c) for c in counts]
    coeff = subcell_coefficient(kappa)
    levels = []
    for level in range(LEVELS):
        weight_sets = [interp_weights(h) for h in spacing] if level < LEVELS - 1 else None
        diag = assemble(lor_diagonal(coeff, spacing))
        levels.append(
            (coeff, spacing, diag, block_mask(coeff.shape), weight_sets, owned_mask(coeff.shape))
        )
        if level < LEVELS - 1:
            coeff = coarsen(coeff)
            spacing = [h.reshape(-1, 2).sum(axis=1) for h in spacing]

    def operator(field):
        return finest_mask * assemble(stiffness_terms(field, weighted, deriv))

    resid = rhs
    precond = cycle(0, resid, levels)
    image = operator(precond)
    rho_old, curv = inner_pair(resid, precond, image)
    alpha = rho_old / curv
    direction, along = (precond, image)
    iterate = alpha * direction
    resid = resid - alpha * along
    precond = cycle(0, resid, levels)
    image = operator(precond)
    rho_new, curv = inner_pair(resid, precond, image)
    ratio = rho_new / rho_old
    alpha = rho_new / (curv - ratio * rho_new / alpha)
    direction = precond + ratio * direction
    along = image + ratio * along
    iterate = iterate + alpha * direction
    resid = resid - alpha * along
    return (iterate[1:, 1:, 1:], resid[1:, 1:, 1:])


def host_tables():
    points = np.array([-1.0, -math.sqrt(3.0 / 7.0), 0.0, math.sqrt(3.0 / 7.0), 1.0])
    quad = np.array([0.1, 49.0 / 90.0, 32.0 / 45.0, 49.0 / 90.0, 0.1])
    bary = np.array(
        [np.prod([points[i] - points[k] for k in range(5) if k != i]) for i in range(5)]
    )
    deriv = np.zeros((5, 5))
    for i in range(5):
        for j in range(5):
            if i != j:
                deriv[i, j] = bary[i] / (bary[j] * (points[i] - points[j]))
    for i in range(5):
        deriv[i, i] = -np.sum(deriv[i])
    deriv[2, 2] = 0.0
    return points, quad, deriv


POINTS, QUAD, DERIV = host_tables()
GAPS = [float(v) for v in POINTS[1:] - POINTS[:-1]]
WIDTHS = [GAPS]
while len(WIDTHS) < LEVELS:
    last = WIDTHS[-1]
    WIDTHS.append([last[2 * i] + last[2 * i + 1] for i in range(len(last) // 2)])


def apply_odd(matrix, u):
    e0, e1, o0, o1 = u[0] + u[4], u[1] + u[3], u[0] - u[4], u[1] - u[3]
    out = [None] * 5
    for i in range(2):
        row = matrix[i]
        p = (
            float(0.5 * (row[0] + row[4])) * e0
            + float(0.5 * (row[1] + row[3])) * e1
            + float(row[2]) * u[2]
        )
        q = float(0.5 * (row[0] - row[4])) * o0 + float(0.5 * (row[1] - row[3])) * o1
        out[i] = q + p
        out[4 - i] = q - p
    out[2] = float(matrix[2][0]) * o0 + float(matrix[2][1]) * o1
    return out


def line_terms(u, w):
    grad = apply_odd(DERIV, u)
    return apply_odd(DERIV.T, [w[i] * grad[i] for i in range(5)])


def plane_terms(v0, v1, coef, hx, inv_hx, widths):
    n = len(widths)
    quarter, twelfth = hx * 0.25, hx * (1.0 / 12.0)
    cache = {}

    def weights(hy, hz):
        key = (round(hy, 12), round(hz, 12))
        if key not in cache:
            m = [[hy / 4 * hz / 4, hy / 4 * hz / 12], [hy / 12 * hz / 4, hy / 12 * hz / 12]]
            k = [
                [0.0, hy / 4 / hz],
                [hz / 4 / hy, hz / 12 / hy + hy / 12 / hz],
            ]
            cache[key] = (
                [[quarter * k[j][l] for l in range(2)] for j in range(2)],
                [[inv_hx * m[j][l] + twelfth * k[j][l] for l in range(2)] for j in range(2)],
            )
        return cache[key]

    near, far = {}, {}

    def add(store, key, value):
        store[key] = store[key] + value if key in store else value

    sums = {k: v0[k] + v1[k] for k in v0}
    diffs = {k: v0[k] - v1[k] for k in v0}
    back = [{}, {}]
    for b in range(n):
        line = {}
        for c in range(n):
            for xi, field in ((0, sums), (1, diffs)):
                lo, hi = (field[b, c], field[b + 1, c]), None
                ys = []
                for cc in (c, c + 1):
                    key = (xi, cc)
                    if key not in line:
                        line[key] = (
                            field[b, cc] + field[b + 1, cc],
                            field[b, cc] - field[b + 1, cc],
                        )
        zline = {}
        for c in range(n):
            ws, wd = weights(widths[b], widths[c])
            value = coef(b, c)
            for xi, w in ((0, ws), (1, wd)):
                for yi in range(2):
                    left, right = line[xi, c][yi], line[xi, c + 1][yi]
                    d = (w[yi][1] * value) * (left - right)
                    if xi == 0 and yi == 0:
                        add(zline, (xi, yi, c), d)
                        add(zline, (xi, yi, c + 1), -d)
                    else:
                        s = (w[yi][0] * value) * (left + right)
                        add(zline, (xi, yi, c), s + d)
                        add(zline, (xi, yi, c + 1), s - d)
        for c in range(n + 1):
            for xi in range(2):
                s, d = zline[xi, 0, c], zline[xi, 1, c]
                add(back[xi], (b, c), s + d)
                add(back[xi], (b + 1, c), s - d)
    for key in back[0]:
        near[key] = back[0][key] + back[1][key]
        far[key] = back[0][key] - back[1][key]
    return near, far


def replicated_kernel(
    ny, where_ref, kappa_ref, source_ref, solution_ref, residual_ref,
    weighted, expanded, out, coeff, winv, resid, guess, direction, iterate,
):
    rows, lanes = kappa_ref.shape[3:]
    halves = rows // 8

    def next_x(t):
        return pltpu.roll(t, rows - ny, 0)

    def next_y(t):
        return pltpu.roll(t, rows - 1, 0)

    def next_z(t):
        return pltpu.roll(t, lanes - 1, 1)

    def prev_x(t):
        return pltpu.roll(t, ny, 0)

    def prev_y(t):
        return pltpu.roll(t, 1, 0)

    def prev_z(t):
        return pltpu.roll(t, 1, 1)

    row = lax.broadcasted_iota(jnp.int32, (rows, lanes), 0)
    lane = lax.broadcasted_iota(jnp.int32, (rows, lanes), 1)
    keep_x = (row >= ny).astype(jnp.float32)
    keep_y = (lax.rem(row, ny) > 0).astype(jnp.float32)
    keep_z = (lane > 0).astype(jnp.float32)

    def masked(a, b, c, t):
        if a == 0:
            t = t * keep_x
        if b == 0:
            t = t * keep_y
        if c == 0:
            t = t * keep_z
        return t

    def phases(n):
        return [(a, b, c) for a in range(n) for b in range(n) for c in range(n)]

    def expand(n, get, put):
        for a in range(n):
            for b in range(n):
                put((a, b, n), next_z(get((a, b, 0))))
        for a in range(n):
            for c in range(n + 1):
                put((a, n, c), next_y(get((a, 0, c))))
        for b in range(n + 1):
            for c in range(n + 1):
                put((n, b, c), next_x(get((0, b, c))))

    def fold(n, get, put):
        for b in range(n + 1):
            for c in range(n + 1):
                put((0, b, c), get((0, b, c)) + prev_x(get((n, b, c))))
        for a in range(n):
            for c in range(n + 1):
                put((a, 0, c), get((a, 0, c)) + prev_y(get((a, n, c))))
        for a in range(n):
            for b in range(n):
                put((a, b, 0), get((a, b, 0)) + prev_z(get((a, b, n))))

    def put_in(ref):
        def put(k, t):
            ref[k] = t
        return put

    def get_from(ref):
        return lambda k: ref[k]

    for a in range(5):
        for b in range(5):
            for c in range(5):
                w = float(QUAD[a] * QUAD[b] * QUAD[c])
                weighted[a, b, c] = w * kappa_ref[a, b, c]
                out[a, b, c] = w * source_ref[a, b, c]
    fold(4, get_from(out), put_in(out))
    for k in phases(4):
        resid[k] = masked(*k, out[k])
        direction[k] = jnp.zeros((rows, lanes), jnp.float32)
        iterate[k] = jnp.zeros((rows, lanes), jnp.float32)

    def pair_z(h):
        i, _ = h
        return i

    for a in range(4):
        two = {
            (b, c): kappa_ref[a, b, c] + kappa_ref[a + 1, b, c]
            for b in range(5) for c in range(5)
        }
        two = {(b, c): two[b, c] + two[b + 1, c] for b in range(4) for c in range(5)}
        for b in range(4):
            for c in range(4):
                coeff[a, b, c] = 0.125 * (two[b, c] + two[b, c + 1])

    def halved(n, get):
        result = {}
        for a, b, c in phases(n // 2):
            t = None
            for x in range(2):
                for y in range(2):
                    for z in range(2):
                        v = get((2 * a + x, 2 * b + y, 2 * c + z))
                        t = v if t is None else t + v
            result[a, b, c] = 0.125 * t
        return result

    coeff1 = halved(4, get_from(coeff))
    coeff2 = halved(2, coeff1.__getitem__)

    def inverse_diagonal(n, widths, get, put):
        cells = {}
        for a, b, c in phases(n):
            x, y, z = widths[a], widths[b], widths[c]
            cells[a, b, c] = get((a, b, c)) * (
                y * z / (9.0 * x) + x * z / (9.0 * y) + x * y / (9.0 * z)
            )
        for axis, prev in ((0, prev_x), (1, prev_y), (2, prev_z)):
            sums = {}
            for k in phases(n):
                lower = list(k)
                lower[axis] = (k[axis] - 1) % n
                t = cells[tuple(lower)]
                sums[k] = cells[k] + (prev(t) if k[axis] == 0 else t)
            cells = sums
        for k in phases(n):
            put(k, masked(*k, relax_weight / cells[k]))

    inverse_diagonal(4, WIDTHS[0], get_from(coeff), put_in(winv))
    winv1, winv2 = {}, {}
    inverse_diagonal(2, WIDTHS[1], coeff1.__getitem__, winv1.__setitem__)
    inverse_diagonal(1, WIDTHS[2], coeff2.__getitem__, winv2.__setitem__)

    def lor_fine():
        expand(4, get_from(expanded), put_in(expanded))
        for b in range(5):
            for c in range(5):
                out[0, b, c] = jnp.zeros((rows, lanes), jnp.float32)

        def step(i, carry):
            a = lax.rem(i, 4)
            part = pl.ds(pl.multiple_of((i // 4) * 8, 8), 8)
            outer = (a == 0) | (a == 3)
            hx = jnp.where(outer, GAPS[0], GAPS[1])
            inv_hx = jnp.where(outer, 1.0 / GAPS[0], 1.0 / GAPS[1])
            keys = [(b, c) for b in range(5) for c in range(5)]
            v0 = {k: expanded[a, k[0], k[1], part, :] for k in keys}
            v1 = {k: expanded[a + 1, k[0], k[1], part, :] for k in keys}
            near, far = plane_terms(
                v0, v1, lambda b, c: coeff[a, b, c, part, :], hx, inv_hx, GAPS
            )
            for b, c in keys:
                out[a, b, c, part, :] += near[b, c]
                out[a + 1, b, c, part, :] = far[b, c]
            return carry

        lax.fori_loop(0, 4 * halves, step, 0)
        fold(4, get_from(out), put_in(out))

    def lor_coarse(field, n, widths, coefs):
        v = dict(field)
        expand(n, v.__getitem__, v.__setitem__)
        total = {}
        for a in range(n):
            keys = [(b, c) for b in range(n + 1) for c in range(n + 1)]
            near, far = plane_terms(
                {k: v[(a,) + k] for k in keys},
                {k: v[(a + 1,) + k] for k in keys},
                lambda b, c: coefs[a, b, c],
                widths[a],
                1.0 / widths[a],
                widths,
            )
            for k in keys:
                key = (a,) + k
                total[key] = total[key] + near[k] if key in total else near[k]
                total[(a + 1,) + k] = far[k]
        fold(n, total.__getitem__, total.__setitem__)
        return total

    def shares(widths):
        left, right = [], []
        for i in range(len(widths) // 2):
            span = widths[2 * i] + widths[2 * i + 1]
            left.append(widths[2 * i + 1] / span)
            right.append(widths[2 * i] / span)
        return left, right

    def restrict_phases(field, n, widths):
        left, right = shares(widths)
        half = n // 2
        sizes = [n, n, n]
        for axis, prev in ((2, prev_z), (1, prev_y), (0, prev_x)):
            sizes[axis] = half
            coarse = {}
            for a in range(sizes[0]):
                for b in range(sizes[1]):
                    for c in range(sizes[2]):
                        k = (a, b, c)
                        j = k[axis]

                        def at(i):
                            return field[k[:axis] + (i,) + k[axis + 1:]]

                        if j == 0:
                            before = right[half - 1] * prev(at(n - 1))
                        else:
                            before = right[j - 1] * at(2 * j - 1)
                        coarse[k] = at(2 * j) + left[j] * at(2 * j + 1) + before
            field = coarse
        return field

    def prolong_phases(field, n, widths):
        left, right = shares(widths)
        half = n // 2
        sizes = [half, half, half]
        for axis, following in ((0, next_x), (1, next_y), (2, next_z)):
            sizes[axis] = n
            fine = {}
            for a in range(sizes[0]):
                for b in range(sizes[1]):
                    for c in range(sizes[2]):
                        k = (a, b, c)
                        i, odd = divmod(k[axis], 2)

                        def at(j):
                            return field[k[:axis] + (j,) + k[axis + 1:]]

                        if odd:
                            after = following(at(0)) if i + 1 == half else at(i + 1)
                            fine[k] = left[i] * at(i) + right[i] * after
                        else:
                            fine[k] = at(i)
            field = fine
        return field

    def precondition():
        for k in phases(4):
            t = winv[k] * resid[k]
            guess[k] = t
            expanded[k] = t
        lor_fine()
        defect = {k: resid[k] - out[k] for k in phases(4)}
        f1 = restrict_phases(defect, 4, WIDTHS[0])
        g1 = {k: winv1[k] * f1[k] for k in f1}
        l1 = lor_coarse(g1, 2, WIDTHS[1], coeff1)
        f2 = restrict_phases({k: f1[k] - l1[k] for k in f1}, 2, WIDTHS[1])
        g2 = {k: winv2[k] * f2[k] for k in f2}
        l2 = lor_coarse(g2, 1, WIDTHS[2], coeff2)
        g2 = {k: g2[k] + winv2[k] * (f2[k] - l2[k]) for k in f2}
        p1 = prolong_phases(g2, 2, WIDTHS[1])
        g1 = {k: g1[k] + p1[k] for k in f1}
        l1 = lor_coarse(g1, 2, WIDTHS[1], coeff1)
        g1 = {k: g1[k] + winv1[k] * (f1[k] - l1[k]) for k in f1}
        p0 = prolong_phases(g1, 4, WIDTHS[0])
        for k in phases(4):
            t = guess[k] + p0[k]
            guess[k] = t
            expanded[k] = t
        lor_fine()

    def operator():
        expand(4, get_from(expanded), put_in(expanded))

        def plane(i, carry):
            a = lax.rem(i, 5)
            part = pl.ds(pl.multiple_of((i // 5) * 8, 8), 8)
            total = {}
            u = {(b, c): expanded[a, b, c, part, :] for b in range(5) for c in range(5)}
            w = {(b, c): weighted[a, b, c, part, :] for b in range(5) for c in range(5)}
            for c in range(5):
                y = line_terms([u[b, c] for b in range(5)], [w[b, c] for b in range(5)])
                for b in range(5):
                    total[b, c] = y[b]
            for b in range(5):
                y = line_terms([u[b, c] for c in range(5)], [w[b, c] for c in range(5)])
                for c in range(5):
                    out[a, b, c, part, :] = total[b, c] + y[c]
            return carry

        lax.fori_loop(0, 5 * halves, plane, 0)

        def columns(i, carry):
            b = lax.rem(i, 5)
            part = pl.ds(pl.multiple_of((i // 5) * 8, 8), 8)
            for c in range(5):
                y = line_terms(
                    [expanded[a, b, c, part, :] for a in range(5)],
                    [weighted[a, b, c, part, :] for a in range(5)],
                )
                for a in range(5):
                    out[a, b, c, part, :] += y[a]
            return carry

        lax.fori_loop(0, 5 * halves, columns, 0)
        fold(4, get_from(out), put_in(out))

    def iteration(_, rho_old):
        precondition()
        total = jnp.zeros((rows, lanes), jnp.float32)
        for k in phases(4):
            r = resid[k]
            z = guess[k] + winv[k] * (r - out[k])
            guess[k] = z
            total = total + r * z
        rho = jnp.sum(total, axis=(0, 1), keepdims=True)
        beta = rho / rho_old
        for k in phases(4):
            p = guess[k] + beta * direction[k]
            direction[k] = p
            expanded[k] = p
        operator()
        total = jnp.zeros((rows, lanes), jnp.float32)
        for k in phases(4):
            total = total + direction[k] * out[k]
        alpha = rho / jnp.sum(total, axis=(0, 1), keepdims=True)
        for k in phases(4):
            iterate[k] += alpha * direction[k]
            resid[k] -= masked(*k, alpha * out[k])
        return rho

    lax.fori_loop(0, 2, iteration, jnp.ones((1, 1), jnp.float32))

    base = where_ref[0]
    for field, result in ((iterate, solution_ref), (resid, residual_ref)):
        for a in range(1, 5):
            for b in range(1, 5):
                at = lax.rem(base + (a // 4) * ny + b // 4, rows)
                for c in range(4):
                    slot = (c + 3) % 4
                    result[slot, pl.ds(4 * (a - 1) + b - 1, 1), :] = field[
                        a % 4, b % 4, c, pl.ds(at, 1), :
                    ]
        result[3] = next_z(result[3])


def replicated_body(kappa, source):
    local = kappa.shape[5]

    def gathered(t):
        flat = t.reshape(125, local)
        whole = lax.all_gather(flat, ("gx", "gy", "gz"))
        nx, ny, nz = (lax.axis_size(name) for name in ("gx", "gy", "gz"))
        whole = whole.reshape(nx * ny, nz, 125, local)
        return jnp.transpose(whole, (2, 0, 1, 3)).reshape(5, 5, 5, nx * ny, nz * local)

    ny = lax.axis_size("gy")
    kappa, source = gathered(kappa), gathered(source)
    rows, lanes = kappa.shape[3:]
    where = (lax.axis_index("gx") * ny + lax.axis_index("gy")).reshape(1).astype(jnp.int32)
    vmem = pl.BlockSpec(memory_space=pltpu.VMEM)

    def field(n):
        return pltpu.VMEM((n, n, n, rows, lanes), jnp.float32)

    outs = pl.pallas_call(
        lambda *refs: replicated_kernel(ny, *refs),
        out_shape=[jax.ShapeDtypeStruct((4, 16, lanes), jnp.float32)] * 2,
        in_specs=[pl.BlockSpec(memory_space=pltpu.SMEM), vmem, vmem],
        out_specs=[vmem, vmem],
        scratch_shapes=[field(5), field(5), field(5)] + [field(4)] * 6,
        name="replicated",
    )(where, kappa, source)

    def own(t):
        t = lax.dynamic_slice_in_dim(t, lax.axis_index("gz") * local, local, axis=2)
        return jnp.transpose(t, (1, 2, 0)).reshape(4, 4, 4 * local)

    return own(outs[0]), own(outs[1])


def body(kappa, source):
    nx, ny, nz = (lax.axis_size(name) for name in ("gx", "gy", "gz"))
    local_x, local_y, local_z = kappa.shape[3:]
    rows, lanes = nx * local_x * ny * local_y, nz * local_z
    small = rows % 8 == 0 and lanes % 128 == 0 and rows * lanes <= 8192
    if local_x == 1 and local_y == 1 and small:
        return replicated_body(kappa, source)
    return distributed_body(kappa, source)


def solution(mesh):
    placed = (P(None, None, None, "gx", "gy", "gz"), P(None, None, None, "gx", "gy", "gz"))
    return jax.shard_map(
        body,
        mesh=mesh,
        in_specs=placed,
        out_specs=(P("gx", "gy", "gz"), P("gx", "gy", "gz")),
        check_vma=False,
    )
```

```python
import math

import jax
import jax.numpy as jnp
import numpy as np
from jax import lax
from jax.experimental import pallas as pl
from jax.experimental.pallas import tpu as pltpu
from jax.sharding import PartitionSpec as P

LEVELS = 3


relax_weight = 0.6


def extended(cells, sides, width):
    for axis, dim in sides:
        count = lax.axis_size(axis)
        ends = count - 1
        head = lax.slice_in_dim(cells, 0, width, axis=dim)
        tail = lax.slice_in_dim(cells, cells.shape[dim] - width, cells.shape[dim], axis=dim)
        cells = jnp.concatenate(
            [
                lax.ppermute(tail, axis, [(i, (i + 1) % count) for i in range(ends)]),
                cells,
                lax.ppermute(head, axis, [((i + 1) % count, i) for i in range(ends)]),
            ],
            axis=dim,
        )
    return cells


def gll_tables():
    points = np.array([-1.0, -math.sqrt(3.0 / 7.0), 0.0, math.sqrt(3.0 / 7.0), 1.0])
    quad_weights = np.array([0.1, 49.0 / 90.0, 32.0 / 45.0, 49.0 / 90.0, 0.1])
    bary = np.array(
        [np.prod([points[i] - points[k] for k in range(5) if k != i]) for i in range(5)]
    )
    deriv = np.zeros((5, 5))
    for i in range(5):
        for j in range(5):
            if i != j:
                deriv[i, j] = bary[i] / (bary[j] * (points[i] - points[j]))
    for i in range(5):
        deriv[i, i] = -np.sum(deriv[i])
    return (
        jnp.asarray(points, jnp.float32),
        jnp.asarray(quad_weights, jnp.float32),
        jnp.asarray(deriv, jnp.float32),
    )


def split_first(values):
    count = (values.shape[0] - 1) // 4
    lower = jnp.swapaxes(values[:-1].reshape((count, 4) + values.shape[1:]), 0, 1)
    return jnp.concatenate([lower, values[4::4][None]], axis=0)


def merge_first(block):
    count = block.shape[1]
    rest = block.shape[2:]
    lower = jnp.swapaxes(block[:4], 0, 1).reshape((4 * count,) + rest)
    tail = jnp.concatenate([jnp.zeros((count, 3) + rest, block.dtype), block[4][:, None]], axis=1)
    tail = tail.reshape((4 * count,) + rest)
    spare = [(0, 0)] * len(rest)
    return jnp.pad(lower, [(0, 1)] + spare) + jnp.pad(tail, [(1, 0)] + spare)


def element_view(field):
    element_portion = split_first(field)
    element_portion = split_first(jnp.moveaxis(element_portion, 2, 0))
    element_portion = split_first(jnp.moveaxis(element_portion, 4, 0))
    return jnp.transpose(element_portion, (4, 2, 0, 5, 3, 1))


def node_sum(block):
    element_portion = jnp.transpose(block, (2, 5, 1, 4, 0, 3))
    element_portion = jnp.moveaxis(merge_first(element_portion), 0, 4)
    element_portion = jnp.moveaxis(merge_first(element_portion), 0, 2)
    return merge_first(element_portion)


def stiffness_terms(field, weighted, deriv):
    highest = lax.Precision.HIGHEST
    local = element_view(field)
    grad_x = jnp.einsum("ia,abcxyz->ibcxyz", deriv, local, precision=highest)
    grad_y = jnp.einsum("jb,abcxyz->ajcxyz", deriv, local, precision=highest)
    grad_z = jnp.einsum("kc,abcxyz->abkxyz", deriv, local, precision=highest)
    back = jnp.einsum("ia,ibcxyz->abcxyz", deriv, weighted * grad_x, precision=highest)
    back = back + jnp.einsum("jb,ajcxyz->abcxyz", deriv, weighted * grad_y, precision=highest)
    back = back + jnp.einsum("kc,abkxyz->abcxyz", deriv, weighted * grad_z, precision=highest)
    return node_sum(back)


def mass_pair(paired, width):
    return jnp.stack(
        [width / 6.0 * (2.0 * paired[0] + paired[1]), width / 6.0 * (paired[0] + 2.0 * paired[1])]
    )


def stiff_pair(paired, width):
    slope = (paired[0] - paired[1]) / width
    return jnp.stack([slope, -slope])


def lor_terms(field, coeff, spacing):
    width_x, width_y, width_z = spacing
    zpairs = jnp.stack([field[:, :, :-1], field[:, :, 1:]])
    zmass = mass_pair(zpairs, width_z)
    stiffness_along_z = stiff_pair(zpairs, width_z)
    ymass = jnp.stack([zmass[:, :, :-1], zmass[:, :, 1:]])
    ystiff = jnp.stack([stiffness_along_z[:, :, :-1], stiffness_along_z[:, :, 1:]])
    column_y = width_y[:, None]
    first = mass_pair(ymass, column_y)
    second = stiff_pair(ymass, column_y) + mass_pair(ystiff, column_y)
    column_x = width_x[:, None, None]
    xfirst = jnp.stack([first[:, :, :-1], first[:, :, 1:]])
    xsecond = jnp.stack([second[:, :, :-1], second[:, :, 1:]])
    cells = (stiff_pair(xfirst, column_x) + mass_pair(xsecond, column_x)) * coeff
    total = jnp.zeros(field.shape, jnp.float32)
    for a in range(2):
        for b in range(2):
            for c in range(2):
                total = total + jnp.pad(cells[a, b, c], ((a, 1 - a), (b, 1 - b), (c, 1 - c)))
    return total


def lor_diagonal(coeff, spacing):
    width_x = spacing[0][:, None, None]
    width_y = spacing[1][None, :, None]
    width_z = spacing[2][None, None, :]
    cells = coeff * (
        width_y * width_z / (9.0 * width_x)
        + width_x * width_z / (9.0 * width_y)
        + width_x * width_y / (9.0 * width_z)
    )
    shape = tuple((n + 1 for n in coeff.shape))
    total = jnp.zeros(shape, jnp.float32)
    for a in range(2):
        for b in range(2):
            for c in range(2):
                total = total + jnp.pad(cells, ((a, 1 - a), (b, 1 - b), (c, 1 - c)))
    return total


def subcell_coefficient(kappa):
    averaged = 0.5 * (kappa[:-1] + kappa[1:])
    averaged = 0.5 * (averaged[:, :-1] + averaged[:, 1:])
    averaged = 0.5 * (averaged[:, :, :-1] + averaged[:, :, 1:])
    count_x, count_y, count_z = averaged.shape[3:]
    return jnp.transpose(averaged, (3, 0, 4, 1, 5, 2)).reshape(
        4 * count_x, 4 * count_y, 4 * count_z
    )


def coarsen(coeff):
    nx, ny, nz = coeff.shape
    return jnp.mean(coeff.reshape(nx // 2, 2, ny // 2, 2, nz // 2, 2), axis=(1, 3, 5))


def interp_weights(width):
    paired = width.reshape(-1, 2)
    span = paired[:, 0] + paired[:, 1]
    return (paired[:, 1] / span, paired[:, 0] / span)


def prolong_first(coarse, left, right):
    shape = (-1,) + (1,) * (coarse.ndim - 1)
    middle = left.reshape(shape) * coarse[:-1] + right.reshape(shape) * coarse[1:]
    woven = jnp.stack([coarse[:-1], middle], axis=1).reshape(
        (2 * (coarse.shape[0] - 1),) + coarse.shape[1:]
    )
    return jnp.concatenate([woven, coarse[-1:]], axis=0)


def restrict_first(fine, left, right):
    shape = (-1,) + (1,) * (fine.ndim - 1)
    middle = fine[1::2]
    spare = [(0, 0)] * (fine.ndim - 1)
    return (
        fine[0::2]
        + jnp.pad(left.reshape(shape) * middle, [(0, 1)] + spare)
        + jnp.pad(right.reshape(shape) * middle, [(1, 0)] + spare)
    )


def prolong(coarse, weight_sets):
    for axis in range(3):
        left, right = weight_sets[axis]
        coarse = jnp.moveaxis(prolong_first(jnp.moveaxis(coarse, axis, 0), left, right), 0, axis)
    return coarse


def restrict(fine, weight_sets):
    for axis in range(3):
        left, right = weight_sets[axis]
        fine = jnp.moveaxis(restrict_first(jnp.moveaxis(fine, axis, 0), left, right), 0, axis)
    return fine


def collapse_leading(padded):
    inner = padded[1:-1]
    head = inner[0] + padded[0]
    tail = inner[-1] + padded[-1]
    return jnp.concatenate([head[None], inner[1:-1], tail[None]], axis=0)


def fold_axis(padded, axis):
    return jnp.moveaxis(collapse_leading(jnp.moveaxis(padded, axis, 0)), 0, axis)


def assemble(partial_value):
    padded = extended(partial_value, (("gx", 0), ("gy", 1), ("gz", 2)), 1)
    return fold_axis(fold_axis(fold_axis(padded, 0), 1), 2)


def side_mask(cells, position, devices):
    index = position * cells + jnp.arange(cells + 1)
    return ((index > 0) & (index < cells * devices)).astype(jnp.float32)


def block_mask(shape):
    mask_x = side_mask(shape[0], lax.axis_index("gx"), lax.axis_size("gx"))
    mask_y = side_mask(shape[1], lax.axis_index("gy"), lax.axis_size("gy"))
    mask_z = side_mask(shape[2], lax.axis_index("gz"), lax.axis_size("gz"))
    return mask_x[:, None, None] * mask_y[None, :, None] * mask_z[None, None, :]


def owned_mask(shape):
    sides = [(jnp.arange(n + 1) >= 1).astype(jnp.float32) for n in shape]
    return sides[0][:, None, None] * sides[1][None, :, None] * sides[2][None, None, :]


def cycle(level, forcing, levels):
    coeff, spacing, diag, mask, weight_sets, owned = levels[level]
    guess = relax_weight * forcing / diag
    if level == LEVELS - 1:
        guess = (
            guess
            + relax_weight * (forcing - mask * assemble(lor_terms(guess, coeff, spacing))) / diag
        )
        return guess
    defect = forcing * owned - lor_terms(guess, coeff, spacing)
    coarse = levels[level + 1][3] * assemble(restrict(defect, weight_sets))
    guess = guess + prolong(cycle(level + 1, coarse, levels), weight_sets)
    return (
        guess + relax_weight * (forcing - mask * assemble(lor_terms(guess, coeff, spacing))) / diag
    )


def inner_pair(resid, precond, image):
    local_rho = jnp.sum(resid[1:, 1:, 1:] * precond[1:, 1:, 1:])
    local_curv = jnp.sum(precond[1:, 1:, 1:] * image[1:, 1:, 1:])
    return lax.psum((local_rho, local_curv), ("gx", "gy", "gz"))


def distributed_body(kappa, source):
    points, quad_weights, deriv = gll_tables()
    cube = (
        quad_weights[:, None, None] * quad_weights[None, :, None] * quad_weights[None, None, :]
    ).reshape(5, 5, 5, 1, 1, 1)
    weighted = kappa * cube
    counts = kappa.shape[3:]
    finest_mask = block_mask([4 * c for c in counts])
    rhs = finest_mask * assemble(node_sum(cube * source))
    gaps = points[1:] - points[:-1]
    spacing = [jnp.tile(gaps, c) for c in counts]
    coeff = subcell_coefficient(kappa)
    levels = []
    for level in range(LEVELS):
        weight_sets = [interp_weights(h) for h in spacing] if level < LEVELS - 1 else None
        diag = assemble(lor_diagonal(coeff, spacing))
        levels.append(
            (coeff, spacing, diag, block_mask(coeff.shape), weight_sets, owned_mask(coeff.shape))
        )
        if level < LEVELS - 1:
            coeff = coarsen(coeff)
            spacing = [h.reshape(-1, 2).sum(axis=1) for h in spacing]

    def operator(field):
        return finest_mask * assemble(stiffness_terms(field, weighted, deriv))

    resid = rhs
    precond = cycle(0, resid, levels)
    image = operator(precond)
    rho_old, curv = inner_pair(resid, precond, image)
    alpha = rho_old / curv
    direction, along = (precond, image)
    iterate = alpha * direction
    resid = resid - alpha * along
    precond = cycle(0, resid, levels)
    image = operator(precond)
    rho_new, curv = inner_pair(resid, precond, image)
    ratio = rho_new / rho_old
    alpha = rho_new / (curv - ratio * rho_new / alpha)
    direction = precond + ratio * direction
    along = image + ratio * along
    iterate = iterate + alpha * direction
    resid = resid - alpha * along
    return (iterate[1:, 1:, 1:], resid[1:, 1:, 1:])


def host_tables():
    points = np.array([-1.0, -math.sqrt(3.0 / 7.0), 0.0, math.sqrt(3.0 / 7.0), 1.0])
    quad = np.array([0.1, 49.0 / 90.0, 32.0 / 45.0, 49.0 / 90.0, 0.1])
    bary = np.array(
        [np.prod([points[i] - points[k] for k in range(5) if k != i]) for i in range(5)]
    )
    deriv = np.zeros((5, 5))
    for i in range(5):
        for j in range(5):
            if i != j:
                deriv[i, j] = bary[i] / (bary[j] * (points[i] - points[j]))
    for i in range(5):
        deriv[i, i] = -np.sum(deriv[i])
    deriv[2, 2] = 0.0
    return points, quad, deriv


POINTS, QUAD, DERIV = host_tables()
GAPS = [float(v) for v in POINTS[1:] - POINTS[:-1]]
WIDTHS = [GAPS]
while len(WIDTHS) < LEVELS:
    last = WIDTHS[-1]
    WIDTHS.append([last[2 * i] + last[2 * i + 1] for i in range(len(last) // 2)])


def apply_odd(matrix, u):
    e0, e1, o0, o1 = u[0] + u[4], u[1] + u[3], u[0] - u[4], u[1] - u[3]
    out = [None] * 5
    for i in range(2):
        row = matrix[i]
        p = (
            float(0.5 * (row[0] + row[4])) * e0
            + float(0.5 * (row[1] + row[3])) * e1
            + float(row[2]) * u[2]
        )
        q = float(0.5 * (row[0] - row[4])) * o0 + float(0.5 * (row[1] - row[3])) * o1
        out[i] = q + p
        out[4 - i] = q - p
    out[2] = float(matrix[2][0]) * o0 + float(matrix[2][1]) * o1
    return out


def line_terms(u, w):
    grad = apply_odd(DERIV, u)
    return apply_odd(DERIV.T, [w[i] * grad[i] for i in range(5)])


def plane_terms(v0, v1, coef, hx, inv_hx, widths):
    n = len(widths)
    quarter, twelfth = hx * 0.25, hx * (1.0 / 12.0)
    cache = {}

    def weights(hy, hz):
        key = (round(hy, 12), round(hz, 12))
        if key not in cache:
            m = [[hy / 4 * hz / 4, hy / 4 * hz / 12], [hy / 12 * hz / 4, hy / 12 * hz / 12]]
            k = [
                [0.0, hy / 4 / hz],
                [hz / 4 / hy, hz / 12 / hy + hy / 12 / hz],
            ]
            cache[key] = (
                [[quarter * k[j][l] for l in range(2)] for j in range(2)],
                [[inv_hx * m[j][l] + twelfth * k[j][l] for l in range(2)] for j in range(2)],
            )
        return cache[key]

    near, far = {}, {}

    def add(store, key, value):
        store[key] = store[key] + value if key in store else value

    sums = {k: v0[k] + v1[k] for k in v0}
    diffs = {k: v0[k] - v1[k] for k in v0}
    back = [{}, {}]
    for b in range(n):
        line = {}
        for c in range(n):
            for xi, field in ((0, sums), (1, diffs)):
                lo, hi = (field[b, c], field[b + 1, c]), None
                ys = []
                for cc in (c, c + 1):
                    key = (xi, cc)
                    if key not in line:
                        line[key] = (
                            field[b, cc] + field[b + 1, cc],
                            field[b, cc] - field[b + 1, cc],
                        )
        zline = {}
        for c in range(n):
            ws, wd = weights(widths[b], widths[c])
            value = coef(b, c)
            for xi, w in ((0, ws), (1, wd)):
                for yi in range(2):
                    left, right = line[xi, c][yi], line[xi, c + 1][yi]
                    d = (w[yi][1] * value) * (left - right)
                    if xi == 0 and yi == 0:
                        add(zline, (xi, yi, c), d)
                        add(zline, (xi, yi, c + 1), -d)
                    else:
                        s = (w[yi][0] * value) * (left + right)
                        add(zline, (xi, yi, c), s + d)
                        add(zline, (xi, yi, c + 1), s - d)
        for c in range(n + 1):
            for xi in range(2):
                s, d = zline[xi, 0, c], zline[xi, 1, c]
                add(back[xi], (b, c), s + d)
                add(back[xi], (b + 1, c), s - d)
    for key in back[0]:
        near[key] = back[0][key] + back[1][key]
        far[key] = back[0][key] - back[1][key]
    return near, far


def replicated_kernel(
    ny, where_ref, blocks_ref, solution_ref, residual_ref,
    weighted, expanded, out, coeff, winv, resid, guess, direction, iterate,
):
    rows, lanes = weighted.shape[3:]
    halves = rows // 8

    def next_x(t):
        return pltpu.roll(t, rows - ny, 0)

    def next_y(t):
        return pltpu.roll(t, rows - 1, 0)

    def next_z(t):
        return pltpu.roll(t, lanes - 1, 1)

    def prev_x(t):
        return pltpu.roll(t, ny, 0)

    def prev_y(t):
        return pltpu.roll(t, 1, 0)

    def prev_z(t):
        return pltpu.roll(t, 1, 1)

    row = lax.broadcasted_iota(jnp.int32, (rows, lanes), 0)
    lane = lax.broadcasted_iota(jnp.int32, (rows, lanes), 1)
    keep_x = (row >= ny).astype(jnp.float32)
    keep_y = (lax.rem(row, ny) > 0).astype(jnp.float32)
    keep_z = (lane > 0).astype(jnp.float32)

    def masked(a, b, c, t):
        if a == 0:
            t = t * keep_x
        if b == 0:
            t = t * keep_y
        if c == 0:
            t = t * keep_z
        return t

    def phases(n):
        return [(a, b, c) for a in range(n) for b in range(n) for c in range(n)]

    def expand(n, get, put):
        for a in range(n):
            for b in range(n):
                put((a, b, n), next_z(get((a, b, 0))))
        for a in range(n):
            for c in range(n + 1):
                put((a, n, c), next_y(get((a, 0, c))))
        for b in range(n + 1):
            for c in range(n + 1):
                put((n, b, c), next_x(get((0, b, c))))

    def fold(n, get, put):
        for b in range(n + 1):
            for c in range(n + 1):
                put((0, b, c), get((0, b, c)) + prev_x(get((n, b, c))))
        for a in range(n):
            for c in range(n + 1):
                put((a, 0, c), get((a, 0, c)) + prev_y(get((a, n, c))))
        for a in range(n):
            for b in range(n):
                put((a, b, 0), get((a, b, 0)) + prev_z(get((a, b, n))))

    def put_in(ref):
        def put(k, t):
            ref[k] = t
        return put

    def get_from(ref):
        return lambda k: ref[k]

    first = lane < lanes // 2
    for a in range(5):
        for b in range(5):
            for c in range(5):
                w = float(QUAD[a] * QUAD[b] * QUAD[c])
                both = blocks_ref[:, (a * 5 + b) * 5 + c, :]
                lower, higher = both[:rows], both[rows:]
                kappa = jnp.where(first, lower, pltpu.roll(higher, lanes // 2, 1))
                source = jnp.where(first, pltpu.roll(lower, lanes // 2, 1), higher)
                expanded[a, b, c] = kappa
                weighted[a, b, c] = w * kappa
                out[a, b, c] = w * source
    fold(4, get_from(out), put_in(out))
    for k in phases(4):
        resid[k] = masked(*k, out[k])
        direction[k] = jnp.zeros((rows, lanes), jnp.float32)
        iterate[k] = jnp.zeros((rows, lanes), jnp.float32)

    for a in range(4):
        two = {
            (b, c): expanded[a, b, c] + expanded[a + 1, b, c]
            for b in range(5) for c in range(5)
        }
        two = {(b, c): two[b, c] + two[b + 1, c] for b in range(4) for c in range(5)}
        for b in range(4):
            for c in range(4):
                coeff[a, b, c] = 0.125 * (two[b, c] + two[b, c + 1])

    def halved(n, get):
        result = {}
        for a, b, c in phases(n // 2):
            t = None
            for x in range(2):
                for y in range(2):
                    for z in range(2):
                        v = get((2 * a + x, 2 * b + y, 2 * c + z))
                        t = v if t is None else t + v
            result[a, b, c] = 0.125 * t
        return result

    coeff1 = halved(4, get_from(coeff))
    coeff2 = halved(2, coeff1.__getitem__)

    def inverse_diagonal(n, widths, get, put):
        cells = {}
        for a, b, c in phases(n):
            x, y, z = widths[a], widths[b], widths[c]
            cells[a, b, c] = get((a, b, c)) * (
                y * z / (9.0 * x) + x * z / (9.0 * y) + x * y / (9.0 * z)
            )
        for axis, prev in ((0, prev_x), (1, prev_y), (2, prev_z)):
            sums = {}
            for k in phases(n):
                lower = list(k)
                lower[axis] = (k[axis] - 1) % n
                t = cells[tuple(lower)]
                sums[k] = cells[k] + (prev(t) if k[axis] == 0 else t)
            cells = sums
        for k in phases(n):
            put(k, masked(*k, relax_weight / cells[k]))

    inverse_diagonal(4, WIDTHS[0], get_from(coeff), put_in(winv))
    winv1, winv2 = {}, {}
    inverse_diagonal(2, WIDTHS[1], coeff1.__getitem__, winv1.__setitem__)
    inverse_diagonal(1, WIDTHS[2], coeff2.__getitem__, winv2.__setitem__)

    def lor_fine():
        expand(4, get_from(expanded), put_in(expanded))
        for b in range(5):
            for c in range(5):
                out[0, b, c] = jnp.zeros((rows, lanes), jnp.float32)

        def step(i, carry):
            a = lax.rem(i, 4)
            part = pl.ds(pl.multiple_of((i // 4) * 8, 8), 8)
            outer = (a == 0) | (a == 3)
            hx = jnp.where(outer, GAPS[0], GAPS[1])
            inv_hx = jnp.where(outer, 1.0 / GAPS[0], 1.0 / GAPS[1])
            keys = [(b, c) for b in range(5) for c in range(5)]
            v0 = {k: expanded[a, k[0], k[1], part, :] for k in keys}
            v1 = {k: expanded[a + 1, k[0], k[1], part, :] for k in keys}
            near, far = plane_terms(
                v0, v1, lambda b, c: coeff[a, b, c, part, :], hx, inv_hx, GAPS
            )
            for b, c in keys:
                out[a, b, c, part, :] += near[b, c]
                out[a + 1, b, c, part, :] = far[b, c]
            return carry

        lax.fori_loop(0, 4 * halves, step, 0)
        fold(4, get_from(out), put_in(out))

    def lor_coarse(field, n, widths, coefs):
        v = dict(field)
        expand(n, v.__getitem__, v.__setitem__)
        total = {}
        for a in range(n):
            keys = [(b, c) for b in range(n + 1) for c in range(n + 1)]
            near, far = plane_terms(
                {k: v[(a,) + k] for k in keys},
                {k: v[(a + 1,) + k] for k in keys},
                lambda b, c: coefs[a, b, c],
                widths[a],
                1.0 / widths[a],
                widths,
            )
            for k in keys:
                key = (a,) + k
                total[key] = total[key] + near[k] if key in total else near[k]
                total[(a + 1,) + k] = far[k]
        fold(n, total.__getitem__, total.__setitem__)
        return total

    def shares(widths):
        left, right = [], []
        for i in range(len(widths) // 2):
            span = widths[2 * i] + widths[2 * i + 1]
            left.append(widths[2 * i + 1] / span)
            right.append(widths[2 * i] / span)
        return left, right

    def restrict_phases(field, n, widths):
        left, right = shares(widths)
        half = n // 2
        sizes = [n, n, n]
        for axis, prev in ((2, prev_z), (1, prev_y), (0, prev_x)):
            sizes[axis] = half
            coarse = {}
            for a in range(sizes[0]):
                for b in range(sizes[1]):
                    for c in range(sizes[2]):
                        k = (a, b, c)
                        j = k[axis]

                        def at(i):
                            return field[k[:axis] + (i,) + k[axis + 1:]]

                        if j == 0:
                            before = right[half - 1] * prev(at(n - 1))
                        else:
                            before = right[j - 1] * at(2 * j - 1)
                        coarse[k] = at(2 * j) + left[j] * at(2 * j + 1) + before
            field = coarse
        return field

    def prolong_phases(field, n, widths):
        left, right = shares(widths)
        half = n // 2
        sizes = [half, half, half]
        for axis, following in ((0, next_x), (1, next_y), (2, next_z)):
            sizes[axis] = n
            fine = {}
            for a in range(sizes[0]):
                for b in range(sizes[1]):
                    for c in range(sizes[2]):
                        k = (a, b, c)
                        i, odd = divmod(k[axis], 2)

                        def at(j):
                            return field[k[:axis] + (j,) + k[axis + 1:]]

                        if odd:
                            after = following(at(0)) if i + 1 == half else at(i + 1)
                            fine[k] = left[i] * at(i) + right[i] * after
                        else:
                            fine[k] = at(i)
            field = fine
        return field

    def precondition():
        for k in phases(4):
            t = winv[k] * resid[k]
            guess[k] = t
            expanded[k] = t
        lor_fine()
        defect = {k: resid[k] - out[k] for k in phases(4)}
        f1 = restrict_phases(defect, 4, WIDTHS[0])
        g1 = {k: winv1[k] * f1[k] for k in f1}
        l1 = lor_coarse(g1, 2, WIDTHS[1], coeff1)
        f2 = restrict_phases({k: f1[k] - l1[k] for k in f1}, 2, WIDTHS[1])
        g2 = {k: winv2[k] * f2[k] for k in f2}
        l2 = lor_coarse(g2, 1, WIDTHS[2], coeff2)
        g2 = {k: g2[k] + winv2[k] * (f2[k] - l2[k]) for k in f2}
        p1 = prolong_phases(g2, 2, WIDTHS[1])
        g1 = {k: g1[k] + p1[k] for k in f1}
        l1 = lor_coarse(g1, 2, WIDTHS[1], coeff1)
        g1 = {k: g1[k] + winv1[k] * (f1[k] - l1[k]) for k in f1}
        p0 = prolong_phases(g1, 4, WIDTHS[0])
        for k in phases(4):
            t = guess[k] + p0[k]
            guess[k] = t
            expanded[k] = t
        lor_fine()

    def operator():
        expand(4, get_from(expanded), put_in(expanded))

        def plane(i, carry):
            a = lax.rem(i, 5)
            part = pl.ds(pl.multiple_of((i // 5) * 8, 8), 8)
            total = {}
            u = {(b, c): expanded[a, b, c, part, :] for b in range(5) for c in range(5)}
            w = {(b, c): weighted[a, b, c, part, :] for b in range(5) for c in range(5)}
            for c in range(5):
                y = line_terms([u[b, c] for b in range(5)], [w[b, c] for b in range(5)])
                for b in range(5):
                    total[b, c] = y[b]
            for b in range(5):
                y = line_terms([u[b, c] for c in range(5)], [w[b, c] for c in range(5)])
                for c in range(5):
                    out[a, b, c, part, :] = total[b, c] + y[c]
            return carry

        lax.fori_loop(0, 5 * halves, plane, 0)

        def columns(i, carry):
            b = lax.rem(i, 5)
            part = pl.ds(pl.multiple_of((i // 5) * 8, 8), 8)
            for c in range(5):
                y = line_terms(
                    [expanded[a, b, c, part, :] for a in range(5)],
                    [weighted[a, b, c, part, :] for a in range(5)],
                )
                for a in range(5):
                    out[a, b, c, part, :] += y[a]
            return carry

        lax.fori_loop(0, 5 * halves, columns, 0)
        fold(4, get_from(out), put_in(out))

    def iteration(_, rho_old):
        precondition()
        total = jnp.zeros((rows, lanes), jnp.float32)
        for k in phases(4):
            r = resid[k]
            z = guess[k] + winv[k] * (r - out[k])
            guess[k] = z
            total = total + r * z
        rho = jnp.sum(total, axis=(0, 1), keepdims=True)
        beta = rho / rho_old
        for k in phases(4):
            p = guess[k] + beta * direction[k]
            direction[k] = p
            expanded[k] = p
        operator()
        total = jnp.zeros((rows, lanes), jnp.float32)
        for k in phases(4):
            total = total + direction[k] * out[k]
        alpha = rho / jnp.sum(total, axis=(0, 1), keepdims=True)
        for k in phases(4):
            iterate[k] += alpha * direction[k]
            resid[k] -= masked(*k, alpha * out[k])
        return rho

    lax.fori_loop(0, 2, iteration, jnp.ones((1, 1), jnp.float32))

    base = where_ref[0]
    for field, result in ((iterate, solution_ref), (resid, residual_ref)):
        for a in range(1, 5):
            for b in range(1, 5):
                at = lax.rem(base + (a // 4) * ny + b // 4, rows)
                for c in range(4):
                    slot = (c + 3) % 4
                    result[slot, pl.ds(4 * (a - 1) + b - 1, 1), :] = field[
                        a % 4, b % 4, c, pl.ds(at, 1), :
                    ]
        result[3] = next_z(result[3])


def gather_kernel(block_ref, all_ref, own_sem, send_sem, recv_sem):
    gx, gy, gz = (lax.axis_index(name) for name in ("gx", "gy", "gz"))
    nx, ny = lax.axis_size("gx"), lax.axis_size("gy")
    rows = block_ref.shape[0]
    upper = rows // 16 * 8
    mesh_id = pl.DeviceIdType.MESH
    cross_x = lax.rem(gx + 2, nx)
    twin = gx + 1 - 2 * lax.rem(gx, 2)
    cross_z = 1 - gz
    to_x, to_z, to_twin = (cross_x, gy, gz), (gx, gy, cross_z), (twin, gy, gz)
    to_y = [(gx, lax.rem(gy + d, ny), gz) for d in range(1, ny)]

    barrier = pltpu.get_barrier_semaphore()
    peers = to_y + [to_x, to_z, to_twin]
    for peer in peers:
        pl.semaphore_signal(barrier, inc=1, device_id=peer, device_id_type=mesh_id)
    pl.semaphore_wait(barrier, len(peers))

    def slot(z, x, y):
        return (z * nx + x) * ny + y

    started = []

    def send(src, dst, device):
        number = len(started)
        copy = pltpu.make_async_remote_copy(
            src_ref=src,
            dst_ref=dst,
            send_sem=send_sem.at[number],
            recv_sem=recv_sem.at[number],
            device_id=device,
            device_id_type=mesh_id,
        )
        copy.start()
        started.append(copy)
        return copy

    mine = all_ref.at[slot(gz, gx, gy)]
    along = [None] + [send(block_ref, mine, device) for device in to_y]
    own = pltpu.make_async_copy(block_ref, mine, own_sem)
    own.start()
    ys = [lax.rem(gy + ny - d, ny) for d in range(ny)]
    by_x, by_z, by_xz, by_zx, last = {}, {}, {}, {}, []

    def column(d):
        if d:
            along[d].wait_recv()
        here = all_ref.at[slot(gz, gx, ys[d])]
        src = here if d else block_ref
        by_x[d] = send(src, here, to_x)
        by_z[d] = send(src, here, to_z)
        last.append(send(src, here, to_twin))

    def onward(d):
        by_x[d].wait_recv()
        number = slot(gz, cross_x, ys[d])
        part = all_ref.at[number, pl.ds(0, upper)]
        by_xz[d] = send(part, part, to_z)
        last.append(send(all_ref.at[number], all_ref.at[number], to_twin))
        by_z[d].wait_recv()
        number = slot(cross_z, gx, ys[d])
        part = all_ref.at[number, pl.ds(upper, rows - upper)]
        by_zx[d] = send(part, part, to_x)
        last.append(send(all_ref.at[number], all_ref.at[number], to_twin))

    column(0)
    for d in range(1, ny):
        column(d)
        onward(d - 1)
    onward(ny - 1)
    for d in range(ny):
        by_xz[d].wait_recv()
        by_zx[d].wait_recv()
        here = all_ref.at[slot(cross_z, cross_x, ys[d])]
        last.append(send(here, here, to_twin))
    for copy in last:
        copy.wait_recv()
    own.wait()
    for copy in started:
        copy.wait_send()


def replicated_body(kappa, source):
    local = kappa.shape[5]
    nx, ny, nz = (lax.axis_size(name) for name in ("gx", "gy", "gz"))
    vmem = pl.BlockSpec(memory_space=pltpu.VMEM)
    block = jnp.concatenate([kappa.reshape(125, local), source.reshape(125, local)], axis=1)
    copies = (ny - 1) + 8 * ny
    blocks = pl.pallas_call(
        gather_kernel,
        out_shape=jax.ShapeDtypeStruct((nz * nx * ny,) + block.shape, jnp.float32),
        in_specs=[vmem],
        out_specs=vmem,
        scratch_shapes=[
            pltpu.SemaphoreType.DMA,
            pltpu.SemaphoreType.DMA((copies,)),
            pltpu.SemaphoreType.DMA((copies,)),
        ],
        compiler_params=pltpu.CompilerParams(collective_id=0, has_side_effects=True),
        name="gather",
    )(block)
    rows, lanes = nx * ny, nz * local
    where = (lax.axis_index("gx") * ny + lax.axis_index("gy")).reshape(1).astype(jnp.int32)

    def field(n):
        return pltpu.VMEM((n, n, n, rows, lanes), jnp.float32)

    outs = pl.pallas_call(
        lambda *refs: replicated_kernel(ny, *refs),
        out_shape=[jax.ShapeDtypeStruct((4, 16, lanes), jnp.float32)] * 2,
        in_specs=[pl.BlockSpec(memory_space=pltpu.SMEM), vmem],
        out_specs=[vmem, vmem],
        scratch_shapes=[field(5), field(5), field(5)] + [field(4)] * 6,
        name="replicated",
    )(where, blocks)

    def own(t):
        t = lax.dynamic_slice_in_dim(t, lax.axis_index("gz") * local, local, axis=2)
        return jnp.transpose(t, (1, 2, 0)).reshape(4, 4, 4 * local)

    return own(outs[0]), own(outs[1])


def body(kappa, source):
    nx, ny, nz = (lax.axis_size(name) for name in ("gx", "gy", "gz"))
    local_x, local_y, local_z = kappa.shape[3:]
    rows, lanes = nx * ny, nz * local_z
    small = rows % 8 == 0 and lanes == 128 and rows <= 64
    if local_x == 1 and local_y == 1 and nx == 4 and nz == 2 and small:
        return replicated_body(kappa, source)
    return distributed_body(kappa, source)


def solution(mesh):
    placed = (P(None, None, None, "gx", "gy", "gz"), P(None, None, None, "gx", "gy", "gz"))
    return jax.shard_map(
        body,
        mesh=mesh,
        in_specs=placed,
        out_specs=(P("gx", "gy", "gz"), P("gx", "gy", "gz")),
        check_vma=False,
    )
```

```python
import math

import jax
import jax.numpy as jnp
import numpy as np
from jax import lax
from jax.experimental import pallas as pl
from jax.experimental.pallas import tpu as pltpu
from jax.sharding import PartitionSpec as P

LEVELS = 3


relax_weight = 0.6


def extended(cells, sides, width):
    for axis, dim in sides:
        count = lax.axis_size(axis)
        ends = count - 1
        head = lax.slice_in_dim(cells, 0, width, axis=dim)
        tail = lax.slice_in_dim(cells, cells.shape[dim] - width, cells.shape[dim], axis=dim)
        cells = jnp.concatenate(
            [
                lax.ppermute(tail, axis, [(i, (i + 1) % count) for i in range(ends)]),
                cells,
                lax.ppermute(head, axis, [((i + 1) % count, i) for i in range(ends)]),
            ],
            axis=dim,
        )
    return cells


def gll_tables():
    points = np.array([-1.0, -math.sqrt(3.0 / 7.0), 0.0, math.sqrt(3.0 / 7.0), 1.0])
    quad_weights = np.array([0.1, 49.0 / 90.0, 32.0 / 45.0, 49.0 / 90.0, 0.1])
    bary = np.array(
        [np.prod([points[i] - points[k] for k in range(5) if k != i]) for i in range(5)]
    )
    deriv = np.zeros((5, 5))
    for i in range(5):
        for j in range(5):
            if i != j:
                deriv[i, j] = bary[i] / (bary[j] * (points[i] - points[j]))
    for i in range(5):
        deriv[i, i] = -np.sum(deriv[i])
    return (
        jnp.asarray(points, jnp.float32),
        jnp.asarray(quad_weights, jnp.float32),
        jnp.asarray(deriv, jnp.float32),
    )


def split_first(values):
    count = (values.shape[0] - 1) // 4
    lower = jnp.swapaxes(values[:-1].reshape((count, 4) + values.shape[1:]), 0, 1)
    return jnp.concatenate([lower, values[4::4][None]], axis=0)


def merge_first(block):
    count = block.shape[1]
    rest = block.shape[2:]
    lower = jnp.swapaxes(block[:4], 0, 1).reshape((4 * count,) + rest)
    tail = jnp.concatenate([jnp.zeros((count, 3) + rest, block.dtype), block[4][:, None]], axis=1)
    tail = tail.reshape((4 * count,) + rest)
    spare = [(0, 0)] * len(rest)
    return jnp.pad(lower, [(0, 1)] + spare) + jnp.pad(tail, [(1, 0)] + spare)


def element_view(field):
    element_portion = split_first(field)
    element_portion = split_first(jnp.moveaxis(element_portion, 2, 0))
    element_portion = split_first(jnp.moveaxis(element_portion, 4, 0))
    return jnp.transpose(element_portion, (4, 2, 0, 5, 3, 1))


def node_sum(block):
    element_portion = jnp.transpose(block, (2, 5, 1, 4, 0, 3))
    element_portion = jnp.moveaxis(merge_first(element_portion), 0, 4)
    element_portion = jnp.moveaxis(merge_first(element_portion), 0, 2)
    return merge_first(element_portion)


def stiffness_terms(field, weighted, deriv):
    highest = lax.Precision.HIGHEST
    local = element_view(field)
    grad_x = jnp.einsum("ia,abcxyz->ibcxyz", deriv, local, precision=highest)
    grad_y = jnp.einsum("jb,abcxyz->ajcxyz", deriv, local, precision=highest)
    grad_z = jnp.einsum("kc,abcxyz->abkxyz", deriv, local, precision=highest)
    back = jnp.einsum("ia,ibcxyz->abcxyz", deriv, weighted * grad_x, precision=highest)
    back = back + jnp.einsum("jb,ajcxyz->abcxyz", deriv, weighted * grad_y, precision=highest)
    back = back + jnp.einsum("kc,abkxyz->abcxyz", deriv, weighted * grad_z, precision=highest)
    return node_sum(back)


def mass_pair(paired, width):
    return jnp.stack(
        [width / 6.0 * (2.0 * paired[0] + paired[1]), width / 6.0 * (paired[0] + 2.0 * paired[1])]
    )


def stiff_pair(paired, width):
    slope = (paired[0] - paired[1]) / width
    return jnp.stack([slope, -slope])


def lor_terms(field, coeff, spacing):
    width_x, width_y, width_z = spacing
    zpairs = jnp.stack([field[:, :, :-1], field[:, :, 1:]])
    zmass = mass_pair(zpairs, width_z)
    stiffness_along_z = stiff_pair(zpairs, width_z)
    ymass = jnp.stack([zmass[:, :, :-1], zmass[:, :, 1:]])
    ystiff = jnp.stack([stiffness_along_z[:, :, :-1], stiffness_along_z[:, :, 1:]])
    column_y = width_y[:, None]
    first = mass_pair(ymass, column_y)
    second = stiff_pair(ymass, column_y) + mass_pair(ystiff, column_y)
    column_x = width_x[:, None, None]
    xfirst = jnp.stack([first[:, :, :-1], first[:, :, 1:]])
    xsecond = jnp.stack([second[:, :, :-1], second[:, :, 1:]])
    cells = (stiff_pair(xfirst, column_x) + mass_pair(xsecond, column_x)) * coeff
    total = jnp.zeros(field.shape, jnp.float32)
    for a in range(2):
        for b in range(2):
            for c in range(2):
                total = total + jnp.pad(cells[a, b, c], ((a, 1 - a), (b, 1 - b), (c, 1 - c)))
    return total


def lor_diagonal(coeff, spacing):
    width_x = spacing[0][:, None, None]
    width_y = spacing[1][None, :, None]
    width_z = spacing[2][None, None, :]
    cells = coeff * (
        width_y * width_z / (9.0 * width_x)
        + width_x * width_z / (9.0 * width_y)
        + width_x * width_y / (9.0 * width_z)
    )
    shape = tuple((n + 1 for n in coeff.shape))
    total = jnp.zeros(shape, jnp.float32)
    for a in range(2):
        for b in range(2):
            for c in range(2):
                total = total + jnp.pad(cells, ((a, 1 - a), (b, 1 - b), (c, 1 - c)))
    return total


def subcell_coefficient(kappa):
    averaged = 0.5 * (kappa[:-1] + kappa[1:])
    averaged = 0.5 * (averaged[:, :-1] + averaged[:, 1:])
    averaged = 0.5 * (averaged[:, :, :-1] + averaged[:, :, 1:])
    count_x, count_y, count_z = averaged.shape[3:]
    return jnp.transpose(averaged, (3, 0, 4, 1, 5, 2)).reshape(
        4 * count_x, 4 * count_y, 4 * count_z
    )


def coarsen(coeff):
    nx, ny, nz = coeff.shape
    return jnp.mean(coeff.reshape(nx // 2, 2, ny // 2, 2, nz // 2, 2), axis=(1, 3, 5))


def interp_weights(width):
    paired = width.reshape(-1, 2)
    span = paired[:, 0] + paired[:, 1]
    return (paired[:, 1] / span, paired[:, 0] / span)


def prolong_first(coarse, left, right):
    shape = (-1,) + (1,) * (coarse.ndim - 1)
    middle = left.reshape(shape) * coarse[:-1] + right.reshape(shape) * coarse[1:]
    woven = jnp.stack([coarse[:-1], middle], axis=1).reshape(
        (2 * (coarse.shape[0] - 1),) + coarse.shape[1:]
    )
    return jnp.concatenate([woven, coarse[-1:]], axis=0)


def restrict_first(fine, left, right):
    shape = (-1,) + (1,) * (fine.ndim - 1)
    middle = fine[1::2]
    spare = [(0, 0)] * (fine.ndim - 1)
    return (
        fine[0::2]
        + jnp.pad(left.reshape(shape) * middle, [(0, 1)] + spare)
        + jnp.pad(right.reshape(shape) * middle, [(1, 0)] + spare)
    )


def prolong(coarse, weight_sets):
    for axis in range(3):
        left, right = weight_sets[axis]
        coarse = jnp.moveaxis(prolong_first(jnp.moveaxis(coarse, axis, 0), left, right), 0, axis)
    return coarse


def restrict(fine, weight_sets):
    for axis in range(3):
        left, right = weight_sets[axis]
        fine = jnp.moveaxis(restrict_first(jnp.moveaxis(fine, axis, 0), left, right), 0, axis)
    return fine


def collapse_leading(padded):
    inner = padded[1:-1]
    head = inner[0] + padded[0]
    tail = inner[-1] + padded[-1]
    return jnp.concatenate([head[None], inner[1:-1], tail[None]], axis=0)


def fold_axis(padded, axis):
    return jnp.moveaxis(collapse_leading(jnp.moveaxis(padded, axis, 0)), 0, axis)


def assemble(partial_value):
    padded = extended(partial_value, (("gx", 0), ("gy", 1), ("gz", 2)), 1)
    return fold_axis(fold_axis(fold_axis(padded, 0), 1), 2)


def side_mask(cells, position, devices):
    index = position * cells + jnp.arange(cells + 1)
    return ((index > 0) & (index < cells * devices)).astype(jnp.float32)


def block_mask(shape):
    mask_x = side_mask(shape[0], lax.axis_index("gx"), lax.axis_size("gx"))
    mask_y = side_mask(shape[1], lax.axis_index("gy"), lax.axis_size("gy"))
    mask_z = side_mask(shape[2], lax.axis_index("gz"), lax.axis_size("gz"))
    return mask_x[:, None, None] * mask_y[None, :, None] * mask_z[None, None, :]


def owned_mask(shape):
    sides = [(jnp.arange(n + 1) >= 1).astype(jnp.float32) for n in shape]
    return sides[0][:, None, None] * sides[1][None, :, None] * sides[2][None, None, :]


def cycle(level, forcing, levels):
    coeff, spacing, diag, mask, weight_sets, owned = levels[level]
    guess = relax_weight * forcing / diag
    if level == LEVELS - 1:
        guess = (
            guess
            + relax_weight * (forcing - mask * assemble(lor_terms(guess, coeff, spacing))) / diag
        )
        return guess
    defect = forcing * owned - lor_terms(guess, coeff, spacing)
    coarse = levels[level + 1][3] * assemble(restrict(defect, weight_sets))
    guess = guess + prolong(cycle(level + 1, coarse, levels), weight_sets)
    return (
        guess + relax_weight * (forcing - mask * assemble(lor_terms(guess, coeff, spacing))) / diag
    )


def inner_pair(resid, precond, image):
    local_rho = jnp.sum(resid[1:, 1:, 1:] * precond[1:, 1:, 1:])
    local_curv = jnp.sum(precond[1:, 1:, 1:] * image[1:, 1:, 1:])
    return lax.psum((local_rho, local_curv), ("gx", "gy", "gz"))


def distributed_body(kappa, source):
    points, quad_weights, deriv = gll_tables()
    cube = (
        quad_weights[:, None, None] * quad_weights[None, :, None] * quad_weights[None, None, :]
    ).reshape(5, 5, 5, 1, 1, 1)
    weighted = kappa * cube
    counts = kappa.shape[3:]
    finest_mask = block_mask([4 * c for c in counts])
    rhs = finest_mask * assemble(node_sum(cube * source))
    gaps = points[1:] - points[:-1]
    spacing = [jnp.tile(gaps, c) for c in counts]
    coeff = subcell_coefficient(kappa)
    levels = []
    for level in range(LEVELS):
        weight_sets = [interp_weights(h) for h in spacing] if level < LEVELS - 1 else None
        diag = assemble(lor_diagonal(coeff, spacing))
        levels.append(
            (coeff, spacing, diag, block_mask(coeff.shape), weight_sets, owned_mask(coeff.shape))
        )
        if level < LEVELS - 1:
            coeff = coarsen(coeff)
            spacing = [h.reshape(-1, 2).sum(axis=1) for h in spacing]

    def operator(field):
        return finest_mask * assemble(stiffness_terms(field, weighted, deriv))

    resid = rhs
    precond = cycle(0, resid, levels)
    image = operator(precond)
    rho_old, curv = inner_pair(resid, precond, image)
    alpha = rho_old / curv
    direction, along = (precond, image)
    iterate = alpha * direction
    resid = resid - alpha * along
    precond = cycle(0, resid, levels)
    image = operator(precond)
    rho_new, curv = inner_pair(resid, precond, image)
    ratio = rho_new / rho_old
    alpha = rho_new / (curv - ratio * rho_new / alpha)
    direction = precond + ratio * direction
    along = image + ratio * along
    iterate = iterate + alpha * direction
    resid = resid - alpha * along
    return (iterate[1:, 1:, 1:], resid[1:, 1:, 1:])


def host_tables():
    points = np.array([-1.0, -math.sqrt(3.0 / 7.0), 0.0, math.sqrt(3.0 / 7.0), 1.0])
    quad = np.array([0.1, 49.0 / 90.0, 32.0 / 45.0, 49.0 / 90.0, 0.1])
    bary = np.array(
        [np.prod([points[i] - points[k] for k in range(5) if k != i]) for i in range(5)]
    )
    deriv = np.zeros((5, 5))
    for i in range(5):
        for j in range(5):
            if i != j:
                deriv[i, j] = bary[i] / (bary[j] * (points[i] - points[j]))
    for i in range(5):
        deriv[i, i] = -np.sum(deriv[i])
    deriv[2, 2] = 0.0
    return points, quad, deriv


POINTS, QUAD, DERIV = host_tables()
GAPS = [float(v) for v in POINTS[1:] - POINTS[:-1]]
WIDTHS = [GAPS]
while len(WIDTHS) < LEVELS:
    last = WIDTHS[-1]
    WIDTHS.append([last[2 * i] + last[2 * i + 1] for i in range(len(last) // 2)])


def apply_odd(matrix, u):
    e0, e1, o0, o1 = u[0] + u[4], u[1] + u[3], u[0] - u[4], u[1] - u[3]
    out = [None] * 5
    for i in range(2):
        row = matrix[i]
        p = (
            float(0.5 * (row[0] + row[4])) * e0
            + float(0.5 * (row[1] + row[3])) * e1
            + float(row[2]) * u[2]
        )
        q = float(0.5 * (row[0] - row[4])) * o0 + float(0.5 * (row[1] - row[3])) * o1
        out[i] = q + p
        out[4 - i] = q - p
    out[2] = float(matrix[2][0]) * o0 + float(matrix[2][1]) * o1
    return out


def line_terms(u, w):
    grad = apply_odd(DERIV, u)
    return apply_odd(DERIV.T, [w[i] * grad[i] for i in range(5)])


def plane_terms(v0, v1, coef, hx, inv_hx, widths):
    n = len(widths)
    quarter, twelfth = hx * 0.25, hx * (1.0 / 12.0)
    cache = {}

    def weights(hy, hz):
        key = (round(hy, 12), round(hz, 12))
        if key not in cache:
            m = [[hy / 4 * hz / 4, hy / 4 * hz / 12], [hy / 12 * hz / 4, hy / 12 * hz / 12]]
            k = [
                [0.0, hy / 4 / hz],
                [hz / 4 / hy, hz / 12 / hy + hy / 12 / hz],
            ]
            cache[key] = (
                [[quarter * k[j][l] for l in range(2)] for j in range(2)],
                [[inv_hx * m[j][l] + twelfth * k[j][l] for l in range(2)] for j in range(2)],
            )
        return cache[key]

    near, far = {}, {}

    def add(store, key, value):
        store[key] = store[key] + value if key in store else value

    sums = {k: v0[k] + v1[k] for k in v0}
    diffs = {k: v0[k] - v1[k] for k in v0}
    back = [{}, {}]
    for b in range(n):
        line = {}
        for c in range(n):
            for xi, field in ((0, sums), (1, diffs)):
                lo, hi = (field[b, c], field[b + 1, c]), None
                ys = []
                for cc in (c, c + 1):
                    key = (xi, cc)
                    if key not in line:
                        line[key] = (
                            field[b, cc] + field[b + 1, cc],
                            field[b, cc] - field[b + 1, cc],
                        )
        zline = {}
        for c in range(n):
            ws, wd = weights(widths[b], widths[c])
            value = coef(b, c)
            for xi, w in ((0, ws), (1, wd)):
                for yi in range(2):
                    left, right = line[xi, c][yi], line[xi, c + 1][yi]
                    d = (w[yi][1] * value) * (left - right)
                    if xi == 0 and yi == 0:
                        add(zline, (xi, yi, c), d)
                        add(zline, (xi, yi, c + 1), -d)
                    else:
                        s = (w[yi][0] * value) * (left + right)
                        add(zline, (xi, yi, c), s + d)
                        add(zline, (xi, yi, c + 1), s - d)
        for c in range(n + 1):
            for xi in range(2):
                s, d = zline[xi, 0, c], zline[xi, 1, c]
                add(back[xi], (b, c), s + d)
                add(back[xi], (b + 1, c), s - d)
    for key in back[0]:
        near[key] = back[0][key] + back[1][key]
        far[key] = back[0][key] - back[1][key]
    return near, far


def replicated_kernel(
    ny, where_ref, blocks_ref, solution_ref, residual_ref,
    weighted, expanded, out, coeff, winv, resid, guess, direction, iterate, picked,
):
    rows, lanes = weighted.shape[3:]
    halves = rows // 8

    def next_x(t):
        return pltpu.roll(t, rows - ny, 0)

    def next_y(t):
        return pltpu.roll(t, rows - 1, 0)

    def next_z(t):
        return pltpu.roll(t, lanes - 1, 1)

    def prev_x(t):
        return pltpu.roll(t, ny, 0)

    def prev_y(t):
        return pltpu.roll(t, 1, 0)

    def prev_z(t):
        return pltpu.roll(t, 1, 1)

    row = lax.broadcasted_iota(jnp.int32, (rows, lanes), 0)
    lane = lax.broadcasted_iota(jnp.int32, (rows, lanes), 1)
    keep_x = (row >= ny).astype(jnp.float32)
    keep_y = (lax.rem(row, ny) > 0).astype(jnp.float32)
    keep_z = (lane > 0).astype(jnp.float32)

    def masked(a, b, c, t):
        if a == 0:
            t = t * keep_x
        if b == 0:
            t = t * keep_y
        if c == 0:
            t = t * keep_z
        return t

    def phases(n):
        return [(a, b, c) for a in range(n) for b in range(n) for c in range(n)]

    def expand(n, get, put):
        for a in range(n):
            for b in range(n):
                put((a, b, n), next_z(get((a, b, 0))))
        for a in range(n):
            for c in range(n + 1):
                put((a, n, c), next_y(get((a, 0, c))))
        for b in range(n + 1):
            for c in range(n + 1):
                put((n, b, c), next_x(get((0, b, c))))

    def fold(n, get, put):
        for b in range(n + 1):
            for c in range(n + 1):
                put((0, b, c), get((0, b, c)) + prev_x(get((n, b, c))))
        for a in range(n):
            for c in range(n + 1):
                put((a, 0, c), get((a, 0, c)) + prev_y(get((a, n, c))))
        for a in range(n):
            for b in range(n):
                put((a, b, 0), get((a, b, 0)) + prev_z(get((a, b, n))))

    def put_in(ref):
        def put(k, t):
            ref[k] = t
        return put

    def get_from(ref):
        return lambda k: ref[k]

    first = lane < lanes // 2
    for a in range(5):
        for b in range(5):
            for c in range(5):
                w = float(QUAD[a] * QUAD[b] * QUAD[c])
                both = blocks_ref[:, (a * 5 + b) * 5 + c, :]
                lower, higher = both[:rows], both[rows:]
                kappa = jnp.where(first, lower, pltpu.roll(higher, lanes // 2, 1))
                source = jnp.where(first, pltpu.roll(lower, lanes // 2, 1), higher)
                expanded[a, b, c] = kappa
                weighted[a, b, c] = w * kappa
                out[a, b, c] = w * source
    fold(4, get_from(out), put_in(out))
    for k in phases(4):
        resid[k] = masked(*k, out[k])
        direction[k] = jnp.zeros((rows, lanes), jnp.float32)
        iterate[k] = jnp.zeros((rows, lanes), jnp.float32)

    for a in range(4):
        two = {
            (b, c): expanded[a, b, c] + expanded[a + 1, b, c]
            for b in range(5) for c in range(5)
        }
        two = {(b, c): two[b, c] + two[b + 1, c] for b in range(4) for c in range(5)}
        for b in range(4):
            for c in range(4):
                coeff[a, b, c] = 0.125 * (two[b, c] + two[b, c + 1])

    def halved(n, get):
        result = {}
        for a, b, c in phases(n // 2):
            t = None
            for x in range(2):
                for y in range(2):
                    for z in range(2):
                        v = get((2 * a + x, 2 * b + y, 2 * c + z))
                        t = v if t is None else t + v
            result[a, b, c] = 0.125 * t
        return result

    coeff1 = halved(4, get_from(coeff))
    coeff2 = halved(2, coeff1.__getitem__)

    def inverse_diagonal(n, widths, get, put):
        cells = {}
        for a, b, c in phases(n):
            x, y, z = widths[a], widths[b], widths[c]
            cells[a, b, c] = get((a, b, c)) * (
                y * z / (9.0 * x) + x * z / (9.0 * y) + x * y / (9.0 * z)
            )
        for axis, prev in ((0, prev_x), (1, prev_y), (2, prev_z)):
            sums = {}
            for k in phases(n):
                lower = list(k)
                lower[axis] = (k[axis] - 1) % n
                t = cells[tuple(lower)]
                sums[k] = cells[k] + (prev(t) if k[axis] == 0 else t)
            cells = sums
        for k in phases(n):
            put(k, masked(*k, relax_weight / cells[k]))

    inverse_diagonal(4, WIDTHS[0], get_from(coeff), put_in(winv))
    winv1, winv2 = {}, {}
    inverse_diagonal(2, WIDTHS[1], coeff1.__getitem__, winv1.__setitem__)
    inverse_diagonal(1, WIDTHS[2], coeff2.__getitem__, winv2.__setitem__)

    def lor_fine():
        expand(4, get_from(expanded), put_in(expanded))
        for b in range(5):
            for c in range(5):
                out[0, b, c] = jnp.zeros((rows, lanes), jnp.float32)

        def step(i, carry):
            a = lax.rem(i, 4)
            part = pl.ds(pl.multiple_of((i // 4) * 8, 8), 8)
            outer = (a == 0) | (a == 3)
            hx = jnp.where(outer, GAPS[0], GAPS[1])
            inv_hx = jnp.where(outer, 1.0 / GAPS[0], 1.0 / GAPS[1])
            keys = [(b, c) for b in range(5) for c in range(5)]
            v0 = {k: expanded[a, k[0], k[1], part, :] for k in keys}
            v1 = {k: expanded[a + 1, k[0], k[1], part, :] for k in keys}
            near, far = plane_terms(
                v0, v1, lambda b, c: coeff[a, b, c, part, :], hx, inv_hx, GAPS
            )
            for b, c in keys:
                out[a, b, c, part, :] += near[b, c]
                out[a + 1, b, c, part, :] = far[b, c]
            return carry

        lax.fori_loop(0, 4 * halves, step, 0)
        fold(4, get_from(out), put_in(out))

    def lor_coarse(field, n, widths, coefs):
        v = dict(field)
        expand(n, v.__getitem__, v.__setitem__)
        total = {}
        for a in range(n):
            keys = [(b, c) for b in range(n + 1) for c in range(n + 1)]
            near, far = plane_terms(
                {k: v[(a,) + k] for k in keys},
                {k: v[(a + 1,) + k] for k in keys},
                lambda b, c: coefs[a, b, c],
                widths[a],
                1.0 / widths[a],
                widths,
            )
            for k in keys:
                key = (a,) + k
                total[key] = total[key] + near[k] if key in total else near[k]
                total[(a + 1,) + k] = far[k]
        fold(n, total.__getitem__, total.__setitem__)
        return total

    def shares(widths):
        left, right = [], []
        for i in range(len(widths) // 2):
            span = widths[2 * i] + widths[2 * i + 1]
            left.append(widths[2 * i + 1] / span)
            right.append(widths[2 * i] / span)
        return left, right

    def restrict_phases(field, n, widths):
        left, right = shares(widths)
        half = n // 2
        sizes = [n, n, n]
        for axis, prev in ((2, prev_z), (1, prev_y), (0, prev_x)):
            sizes[axis] = half
            coarse = {}
            for a in range(sizes[0]):
                for b in range(sizes[1]):
                    for c in range(sizes[2]):
                        k = (a, b, c)
                        j = k[axis]

                        def at(i):
                            return field[k[:axis] + (i,) + k[axis + 1:]]

                        if j == 0:
                            before = right[half - 1] * prev(at(n - 1))
                        else:
                            before = right[j - 1] * at(2 * j - 1)
                        coarse[k] = at(2 * j) + left[j] * at(2 * j + 1) + before
            field = coarse
        return field

    def prolong_phases(field, n, widths):
        left, right = shares(widths)
        half = n // 2
        sizes = [half, half, half]
        for axis, following in ((0, next_x), (1, next_y), (2, next_z)):
            sizes[axis] = n
            fine = {}
            for a in range(sizes[0]):
                for b in range(sizes[1]):
                    for c in range(sizes[2]):
                        k = (a, b, c)
                        i, odd = divmod(k[axis], 2)

                        def at(j):
                            return field[k[:axis] + (j,) + k[axis + 1:]]

                        if odd:
                            after = following(at(0)) if i + 1 == half else at(i + 1)
                            fine[k] = left[i] * at(i) + right[i] * after
                        else:
                            fine[k] = at(i)
            field = fine
        return field

    def precondition():
        for k in phases(4):
            t = winv[k] * resid[k]
            guess[k] = t
            expanded[k] = t
        lor_fine()
        defect = {k: resid[k] - out[k] for k in phases(4)}
        f1 = restrict_phases(defect, 4, WIDTHS[0])
        g1 = {k: winv1[k] * f1[k] for k in f1}
        l1 = lor_coarse(g1, 2, WIDTHS[1], coeff1)
        f2 = restrict_phases({k: f1[k] - l1[k] for k in f1}, 2, WIDTHS[1])
        g2 = {k: winv2[k] * f2[k] for k in f2}
        l2 = lor_coarse(g2, 1, WIDTHS[2], coeff2)
        g2 = {k: g2[k] + winv2[k] * (f2[k] - l2[k]) for k in f2}
        p1 = prolong_phases(g2, 2, WIDTHS[1])
        g1 = {k: g1[k] + p1[k] for k in f1}
        l1 = lor_coarse(g1, 2, WIDTHS[1], coeff1)
        g1 = {k: g1[k] + winv1[k] * (f1[k] - l1[k]) for k in f1}
        p0 = prolong_phases(g1, 4, WIDTHS[0])
        for k in phases(4):
            t = guess[k] + p0[k]
            guess[k] = t
            expanded[k] = t
        lor_fine()

    def operator():
        expand(4, get_from(expanded), put_in(expanded))

        def plane(i, carry):
            a = lax.rem(i, 5)
            part = pl.ds(pl.multiple_of((i // 5) * 8, 8), 8)
            total = {}
            u = {(b, c): expanded[a, b, c, part, :] for b in range(5) for c in range(5)}
            w = {(b, c): weighted[a, b, c, part, :] for b in range(5) for c in range(5)}
            for c in range(5):
                y = line_terms([u[b, c] for b in range(5)], [w[b, c] for b in range(5)])
                for b in range(5):
                    total[b, c] = y[b]
            for b in range(5):
                y = line_terms([u[b, c] for c in range(5)], [w[b, c] for c in range(5)])
                for c in range(5):
                    out[a, b, c, part, :] = total[b, c] + y[c]
            return carry

        lax.fori_loop(0, 5 * halves, plane, 0)

        def columns(i, carry):
            b = lax.rem(i, 5)
            part = pl.ds(pl.multiple_of((i // 5) * 8, 8), 8)
            for c in range(5):
                y = line_terms(
                    [expanded[a, b, c, part, :] for a in range(5)],
                    [weighted[a, b, c, part, :] for a in range(5)],
                )
                for a in range(5):
                    out[a, b, c, part, :] += y[a]
            return carry

        lax.fori_loop(0, 5 * halves, columns, 0)
        fold(4, get_from(out), put_in(out))

    def iteration(_, rho_old):
        precondition()
        total = jnp.zeros((rows, lanes), jnp.float32)
        for k in phases(4):
            r = resid[k]
            z = guess[k] + winv[k] * (r - out[k])
            guess[k] = z
            total = total + r * z
        rho = jnp.sum(total, axis=(0, 1), keepdims=True)
        beta = rho / rho_old
        for k in phases(4):
            p = guess[k] + beta * direction[k]
            direction[k] = p
            expanded[k] = p
        operator()
        total = jnp.zeros((rows, lanes), jnp.float32)
        for k in phases(4):
            total = total + direction[k] * out[k]
        alpha = rho / jnp.sum(total, axis=(0, 1), keepdims=True)
        for k in phases(4):
            iterate[k] += alpha * direction[k]
            resid[k] -= masked(*k, alpha * out[k])
        return rho

    lax.fori_loop(0, 2, iteration, jnp.ones((1, 1), jnp.float32))

    base = where_ref[0]
    for index, field in enumerate((iterate, resid)):
        for a in range(1, 5):
            for b in range(1, 5):
                at = lax.rem(base + (a // 4) * ny + b // 4, rows)
                for c in range(4):
                    picked[c, pl.ds(16 * index + 4 * (a - 1) + b - 1, 1), :] = field[
                        a % 4, b % 4, c, pl.ds(at, 1), :
                    ]
    width = solution_ref.shape[2]
    lane_in = lax.broadcasted_iota(jnp.int32, (lanes, width), 0)
    lane_out = lax.broadcasted_iota(jnp.int32, (lanes, width), 1)
    total = jnp.zeros((32, width), jnp.float32)
    for slot in range(4):
        t = picked[1 + slot] if slot < 3 else next_z(picked[0])
        hot = (lane_out == 4 * (lane_in - where_ref[1]) + slot).astype(jnp.bfloat16)
        high = t.astype(jnp.bfloat16)
        rest = t - high.astype(jnp.float32)
        middle = rest.astype(jnp.bfloat16)
        low = (rest - middle.astype(jnp.float32)).astype(jnp.bfloat16)
        parts = jnp.dot(
            jnp.concatenate([high, middle, low], axis=0), hot,
            preferred_element_type=jnp.float32,
        )
        total = total + ((parts[:32] + parts[32:64]) + parts[64:])
    for i in range(4):
        solution_ref[i] = total[4 * i : 4 * i + 4]
        residual_ref[i] = total[16 + 4 * i : 20 + 4 * i]


def gather_kernel(block_ref, all_ref, own_sem, send_sem, recv_sem):
    gx, gy, gz = (lax.axis_index(name) for name in ("gx", "gy", "gz"))
    nx, ny = lax.axis_size("gx"), lax.axis_size("gy")
    rows = block_ref.shape[0]
    upper = rows // 16 * 8
    mesh_id = pl.DeviceIdType.MESH
    cross_x = lax.rem(gx + 2, nx)
    twin = gx + 1 - 2 * lax.rem(gx, 2)
    cross_z = 1 - gz
    to_x, to_z, to_twin = (cross_x, gy, gz), (gx, gy, cross_z), (twin, gy, gz)
    to_y = [(gx, lax.rem(gy + d, ny), gz) for d in range(1, ny)]

    barrier = pltpu.get_barrier_semaphore()
    peers = to_y + [to_x, to_z, to_twin]
    for peer in peers:
        pl.semaphore_signal(barrier, inc=1, device_id=peer, device_id_type=mesh_id)
    pl.semaphore_wait(barrier, len(peers))

    def slot(z, x, y):
        return (z * nx + x) * ny + y

    started = []

    def send(src, dst, device):
        number = len(started)
        copy = pltpu.make_async_remote_copy(
            src_ref=src,
            dst_ref=dst,
            send_sem=send_sem.at[number],
            recv_sem=recv_sem.at[number],
            device_id=device,
            device_id_type=mesh_id,
        )
        copy.start()
        started.append(copy)
        return copy

    mine = all_ref.at[slot(gz, gx, gy)]
    along = [None] + [send(block_ref, mine, device) for device in to_y]
    own = pltpu.make_async_copy(block_ref, mine, own_sem)
    own.start()
    ys = [lax.rem(gy + ny - d, ny) for d in range(ny)]
    by_x, by_z, by_xz, by_zx, last = {}, {}, {}, {}, []

    def column(d):
        if d:
            along[d].wait_recv()
        here = all_ref.at[slot(gz, gx, ys[d])]
        src = here if d else block_ref
        by_x[d] = send(src, here, to_x)
        by_z[d] = send(src, here, to_z)
        last.append(send(src, here, to_twin))

    def onward(d):
        by_x[d].wait_recv()
        number = slot(gz, cross_x, ys[d])
        part = all_ref.at[number, pl.ds(0, upper)]
        by_xz[d] = send(part, part, to_z)
        last.append(send(all_ref.at[number], all_ref.at[number], to_twin))
        by_z[d].wait_recv()
        number = slot(cross_z, gx, ys[d])
        part = all_ref.at[number, pl.ds(upper, rows - upper)]
        by_zx[d] = send(part, part, to_x)
        last.append(send(all_ref.at[number], all_ref.at[number], to_twin))

    column(0)
    for d in range(1, ny):
        column(d)
        onward(d - 1)
    onward(ny - 1)
    for d in range(ny):
        by_xz[d].wait_recv()
        by_zx[d].wait_recv()
        here = all_ref.at[slot(cross_z, cross_x, ys[d])]
        last.append(send(here, here, to_twin))
    for copy in last:
        copy.wait_recv()
    own.wait()
    for copy in started:
        copy.wait_send()


def replicated_body(kappa, source):
    local = kappa.shape[5]
    nx, ny, nz = (lax.axis_size(name) for name in ("gx", "gy", "gz"))
    vmem = pl.BlockSpec(memory_space=pltpu.VMEM)
    block = jnp.concatenate([kappa, source], axis=5).reshape(125, 2 * local)
    copies = (ny - 1) + 8 * ny
    blocks = pl.pallas_call(
        gather_kernel,
        out_shape=pltpu.VMEM((nz * nx * ny,) + block.shape, jnp.float32),
        in_specs=[vmem],
        out_specs=vmem,
        scratch_shapes=[
            pltpu.SemaphoreType.DMA,
            pltpu.SemaphoreType.DMA((copies,)),
            pltpu.SemaphoreType.DMA((copies,)),
        ],
        compiler_params=pltpu.CompilerParams(collective_id=0, has_side_effects=True),
        name="gather",
    )(block)
    rows, lanes = nx * ny, nz * local
    place = lax.axis_index("gx") * ny + lax.axis_index("gy")
    where = jnp.stack([place, lax.axis_index("gz") * local]).astype(jnp.int32)

    def field(n):
        return pltpu.VMEM((n, n, n, rows, lanes), jnp.float32)

    outs = pl.pallas_call(
        lambda *refs: replicated_kernel(ny, *refs),
        out_shape=[jax.ShapeDtypeStruct((4, 4, 4 * local), jnp.float32)] * 2,
        in_specs=[pl.BlockSpec(memory_space=pltpu.SMEM), vmem],
        out_specs=[vmem, vmem],
        scratch_shapes=[field(5), field(5), field(5)] + [field(4)] * 6
        + [pltpu.VMEM((4, 32, lanes), jnp.float32)],
        name="replicated",
    )(where, pltpu.with_memory_space_constraint(blocks, pltpu.VMEM))

    return outs[0], outs[1]


def body(kappa, source):
    nx, ny, nz = (lax.axis_size(name) for name in ("gx", "gy", "gz"))
    local_x, local_y, local_z = kappa.shape[3:]
    rows, lanes = nx * ny, nz * local_z
    small = rows % 8 == 0 and lanes == 128 and rows <= 64
    if local_x == 1 and local_y == 1 and nx == 4 and nz == 2 and small:
        return replicated_body(kappa, source)
    return distributed_body(kappa, source)


def solution(mesh):
    placed = (P(None, None, None, "gx", "gy", "gz"), P(None, None, None, "gx", "gy", "gz"))
    return jax.shard_map(
        body,
        mesh=mesh,
        in_specs=placed,
        out_specs=(P("gx", "gy", "gz"), P("gx", "gy", "gz")),
        check_vma=False,
    )
```

```python
import math

import jax
import jax.numpy as jnp
import numpy as np
from jax import lax
from jax.experimental import pallas as pl
from jax.experimental.pallas import tpu as pltpu
from jax.sharding import PartitionSpec as P

LEVELS = 3


relax_weight = 0.6


def extended(cells, sides, width):
    for axis, dim in sides:
        count = lax.axis_size(axis)
        ends = count - 1
        head = lax.slice_in_dim(cells, 0, width, axis=dim)
        tail = lax.slice_in_dim(cells, cells.shape[dim] - width, cells.shape[dim], axis=dim)
        cells = jnp.concatenate(
            [
                lax.ppermute(tail, axis, [(i, (i + 1) % count) for i in range(ends)]),
                cells,
                lax.ppermute(head, axis, [((i + 1) % count, i) for i in range(ends)]),
            ],
            axis=dim,
        )
    return cells


def gll_tables():
    points = np.array([-1.0, -math.sqrt(3.0 / 7.0), 0.0, math.sqrt(3.0 / 7.0), 1.0])
    quad_weights = np.array([0.1, 49.0 / 90.0, 32.0 / 45.0, 49.0 / 90.0, 0.1])
    bary = np.array(
        [np.prod([points[i] - points[k] for k in range(5) if k != i]) for i in range(5)]
    )
    deriv = np.zeros((5, 5))
    for i in range(5):
        for j in range(5):
            if i != j:
                deriv[i, j] = bary[i] / (bary[j] * (points[i] - points[j]))
    for i in range(5):
        deriv[i, i] = -np.sum(deriv[i])
    return (
        jnp.asarray(points, jnp.float32),
        jnp.asarray(quad_weights, jnp.float32),
        jnp.asarray(deriv, jnp.float32),
    )


def split_first(values):
    count = (values.shape[0] - 1) // 4
    lower = jnp.swapaxes(values[:-1].reshape((count, 4) + values.shape[1:]), 0, 1)
    return jnp.concatenate([lower, values[4::4][None]], axis=0)


def merge_first(block):
    count = block.shape[1]
    rest = block.shape[2:]
    lower = jnp.swapaxes(block[:4], 0, 1).reshape((4 * count,) + rest)
    tail = jnp.concatenate([jnp.zeros((count, 3) + rest, block.dtype), block[4][:, None]], axis=1)
    tail = tail.reshape((4 * count,) + rest)
    spare = [(0, 0)] * len(rest)
    return jnp.pad(lower, [(0, 1)] + spare) + jnp.pad(tail, [(1, 0)] + spare)


def element_view(field):
    element_portion = split_first(field)
    element_portion = split_first(jnp.moveaxis(element_portion, 2, 0))
    element_portion = split_first(jnp.moveaxis(element_portion, 4, 0))
    return jnp.transpose(element_portion, (4, 2, 0, 5, 3, 1))


def node_sum(block):
    element_portion = jnp.transpose(block, (2, 5, 1, 4, 0, 3))
    element_portion = jnp.moveaxis(merge_first(element_portion), 0, 4)
    element_portion = jnp.moveaxis(merge_first(element_portion), 0, 2)
    return merge_first(element_portion)


def stiffness_terms(field, weighted, deriv):
    highest = lax.Precision.HIGHEST
    local = element_view(field)
    grad_x = jnp.einsum("ia,abcxyz->ibcxyz", deriv, local, precision=highest)
    grad_y = jnp.einsum("jb,abcxyz->ajcxyz", deriv, local, precision=highest)
    grad_z = jnp.einsum("kc,abcxyz->abkxyz", deriv, local, precision=highest)
    back = jnp.einsum("ia,ibcxyz->abcxyz", deriv, weighted * grad_x, precision=highest)
    back = back + jnp.einsum("jb,ajcxyz->abcxyz", deriv, weighted * grad_y, precision=highest)
    back = back + jnp.einsum("kc,abkxyz->abcxyz", deriv, weighted * grad_z, precision=highest)
    return node_sum(back)


def mass_pair(paired, width):
    return jnp.stack(
        [width / 6.0 * (2.0 * paired[0] + paired[1]), width / 6.0 * (paired[0] + 2.0 * paired[1])]
    )


def stiff_pair(paired, width):
    slope = (paired[0] - paired[1]) / width
    return jnp.stack([slope, -slope])


def lor_terms(field, coeff, spacing):
    width_x, width_y, width_z = spacing
    zpairs = jnp.stack([field[:, :, :-1], field[:, :, 1:]])
    zmass = mass_pair(zpairs, width_z)
    stiffness_along_z = stiff_pair(zpairs, width_z)
    ymass = jnp.stack([zmass[:, :, :-1], zmass[:, :, 1:]])
    ystiff = jnp.stack([stiffness_along_z[:, :, :-1], stiffness_along_z[:, :, 1:]])
    column_y = width_y[:, None]
    first = mass_pair(ymass, column_y)
    second = stiff_pair(ymass, column_y) + mass_pair(ystiff, column_y)
    column_x = width_x[:, None, None]
    xfirst = jnp.stack([first[:, :, :-1], first[:, :, 1:]])
    xsecond = jnp.stack([second[:, :, :-1], second[:, :, 1:]])
    cells = (stiff_pair(xfirst, column_x) + mass_pair(xsecond, column_x)) * coeff
    total = jnp.zeros(field.shape, jnp.float32)
    for a in range(2):
        for b in range(2):
            for c in range(2):
                total = total + jnp.pad(cells[a, b, c], ((a, 1 - a), (b, 1 - b), (c, 1 - c)))
    return total


def lor_diagonal(coeff, spacing):
    width_x = spacing[0][:, None, None]
    width_y = spacing[1][None, :, None]
    width_z = spacing[2][None, None, :]
    cells = coeff * (
        width_y * width_z / (9.0 * width_x)
        + width_x * width_z / (9.0 * width_y)
        + width_x * width_y / (9.0 * width_z)
    )
    shape = tuple((n + 1 for n in coeff.shape))
    total = jnp.zeros(shape, jnp.float32)
    for a in range(2):
        for b in range(2):
            for c in range(2):
                total = total + jnp.pad(cells, ((a, 1 - a), (b, 1 - b), (c, 1 - c)))
    return total


def subcell_coefficient(kappa):
    averaged = 0.5 * (kappa[:-1] + kappa[1:])
    averaged = 0.5 * (averaged[:, :-1] + averaged[:, 1:])
    averaged = 0.5 * (averaged[:, :, :-1] + averaged[:, :, 1:])
    count_x, count_y, count_z = averaged.shape[3:]
    return jnp.transpose(averaged, (3, 0, 4, 1, 5, 2)).reshape(
        4 * count_x, 4 * count_y, 4 * count_z
    )


def coarsen(coeff):
    nx, ny, nz = coeff.shape
    return jnp.mean(coeff.reshape(nx // 2, 2, ny // 2, 2, nz // 2, 2), axis=(1, 3, 5))


def interp_weights(width):
    paired = width.reshape(-1, 2)
    span = paired[:, 0] + paired[:, 1]
    return (paired[:, 1] / span, paired[:, 0] / span)


def prolong_first(coarse, left, right):
    shape = (-1,) + (1,) * (coarse.ndim - 1)
    middle = left.reshape(shape) * coarse[:-1] + right.reshape(shape) * coarse[1:]
    woven = jnp.stack([coarse[:-1], middle], axis=1).reshape(
        (2 * (coarse.shape[0] - 1),) + coarse.shape[1:]
    )
    return jnp.concatenate([woven, coarse[-1:]], axis=0)


def restrict_first(fine, left, right):
    shape = (-1,) + (1,) * (fine.ndim - 1)
    middle = fine[1::2]
    spare = [(0, 0)] * (fine.ndim - 1)
    return (
        fine[0::2]
        + jnp.pad(left.reshape(shape) * middle, [(0, 1)] + spare)
        + jnp.pad(right.reshape(shape) * middle, [(1, 0)] + spare)
    )


def prolong(coarse, weight_sets):
    for axis in range(3):
        left, right = weight_sets[axis]
        coarse = jnp.moveaxis(prolong_first(jnp.moveaxis(coarse, axis, 0), left, right), 0, axis)
    return coarse


def restrict(fine, weight_sets):
    for axis in range(3):
        left, right = weight_sets[axis]
        fine = jnp.moveaxis(restrict_first(jnp.moveaxis(fine, axis, 0), left, right), 0, axis)
    return fine


def collapse_leading(padded):
    inner = padded[1:-1]
    head = inner[0] + padded[0]
    tail = inner[-1] + padded[-1]
    return jnp.concatenate([head[None], inner[1:-1], tail[None]], axis=0)


def fold_axis(padded, axis):
    return jnp.moveaxis(collapse_leading(jnp.moveaxis(padded, axis, 0)), 0, axis)


def assemble(partial_value):
    padded = extended(partial_value, (("gx", 0), ("gy", 1), ("gz", 2)), 1)
    return fold_axis(fold_axis(fold_axis(padded, 0), 1), 2)


def side_mask(cells, position, devices):
    index = position * cells + jnp.arange(cells + 1)
    return ((index > 0) & (index < cells * devices)).astype(jnp.float32)


def block_mask(shape):
    mask_x = side_mask(shape[0], lax.axis_index("gx"), lax.axis_size("gx"))
    mask_y = side_mask(shape[1], lax.axis_index("gy"), lax.axis_size("gy"))
    mask_z = side_mask(shape[2], lax.axis_index("gz"), lax.axis_size("gz"))
    return mask_x[:, None, None] * mask_y[None, :, None] * mask_z[None, None, :]


def owned_mask(shape):
    sides = [(jnp.arange(n + 1) >= 1).astype(jnp.float32) for n in shape]
    return sides[0][:, None, None] * sides[1][None, :, None] * sides[2][None, None, :]


def cycle(level, forcing, levels):
    coeff, spacing, diag, mask, weight_sets, owned = levels[level]
    guess = relax_weight * forcing / diag
    if level == LEVELS - 1:
        guess = (
            guess
            + relax_weight * (forcing - mask * assemble(lor_terms(guess, coeff, spacing))) / diag
        )
        return guess
    defect = forcing * owned - lor_terms(guess, coeff, spacing)
    coarse = levels[level + 1][3] * assemble(restrict(defect, weight_sets))
    guess = guess + prolong(cycle(level + 1, coarse, levels), weight_sets)
    return (
        guess + relax_weight * (forcing - mask * assemble(lor_terms(guess, coeff, spacing))) / diag
    )


def inner_pair(resid, precond, image):
    local_rho = jnp.sum(resid[1:, 1:, 1:] * precond[1:, 1:, 1:])
    local_curv = jnp.sum(precond[1:, 1:, 1:] * image[1:, 1:, 1:])
    return lax.psum((local_rho, local_curv), ("gx", "gy", "gz"))


def distributed_body(kappa, source):
    points, quad_weights, deriv = gll_tables()
    cube = (
        quad_weights[:, None, None] * quad_weights[None, :, None] * quad_weights[None, None, :]
    ).reshape(5, 5, 5, 1, 1, 1)
    weighted = kappa * cube
    counts = kappa.shape[3:]
    finest_mask = block_mask([4 * c for c in counts])
    rhs = finest_mask * assemble(node_sum(cube * source))
    gaps = points[1:] - points[:-1]
    spacing = [jnp.tile(gaps, c) for c in counts]
    coeff = subcell_coefficient(kappa)
    levels = []
    for level in range(LEVELS):
        weight_sets = [interp_weights(h) for h in spacing] if level < LEVELS - 1 else None
        diag = assemble(lor_diagonal(coeff, spacing))
        levels.append(
            (coeff, spacing, diag, block_mask(coeff.shape), weight_sets, owned_mask(coeff.shape))
        )
        if level < LEVELS - 1:
            coeff = coarsen(coeff)
            spacing = [h.reshape(-1, 2).sum(axis=1) for h in spacing]

    def operator(field):
        return finest_mask * assemble(stiffness_terms(field, weighted, deriv))

    resid = rhs
    precond = cycle(0, resid, levels)
    image = operator(precond)
    rho_old, curv = inner_pair(resid, precond, image)
    alpha = rho_old / curv
    direction, along = (precond, image)
    iterate = alpha * direction
    resid = resid - alpha * along
    precond = cycle(0, resid, levels)
    image = operator(precond)
    rho_new, curv = inner_pair(resid, precond, image)
    ratio = rho_new / rho_old
    alpha = rho_new / (curv - ratio * rho_new / alpha)
    direction = precond + ratio * direction
    along = image + ratio * along
    iterate = iterate + alpha * direction
    resid = resid - alpha * along
    return (iterate[1:, 1:, 1:], resid[1:, 1:, 1:])


def host_tables():
    points = np.array([-1.0, -math.sqrt(3.0 / 7.0), 0.0, math.sqrt(3.0 / 7.0), 1.0])
    quad = np.array([0.1, 49.0 / 90.0, 32.0 / 45.0, 49.0 / 90.0, 0.1])
    bary = np.array(
        [np.prod([points[i] - points[k] for k in range(5) if k != i]) for i in range(5)]
    )
    deriv = np.zeros((5, 5))
    for i in range(5):
        for j in range(5):
            if i != j:
                deriv[i, j] = bary[i] / (bary[j] * (points[i] - points[j]))
    for i in range(5):
        deriv[i, i] = -np.sum(deriv[i])
    deriv[2, 2] = 0.0
    return points, quad, deriv


POINTS, QUAD, DERIV = host_tables()
GAPS = [float(v) for v in POINTS[1:] - POINTS[:-1]]
WIDTHS = [GAPS]
while len(WIDTHS) < LEVELS:
    last = WIDTHS[-1]
    WIDTHS.append([last[2 * i] + last[2 * i + 1] for i in range(len(last) // 2)])


def apply_odd(matrix, u):
    e0, e1, o0, o1 = u[0] + u[4], u[1] + u[3], u[0] - u[4], u[1] - u[3]
    out = [None] * 5
    for i in range(2):
        row = matrix[i]
        p = (
            float(0.5 * (row[0] + row[4])) * e0
            + float(0.5 * (row[1] + row[3])) * e1
            + float(row[2]) * u[2]
        )
        q = float(0.5 * (row[0] - row[4])) * o0 + float(0.5 * (row[1] - row[3])) * o1
        out[i] = q + p
        out[4 - i] = q - p
    out[2] = float(matrix[2][0]) * o0 + float(matrix[2][1]) * o1
    return out


def line_terms(u, w):
    grad = apply_odd(DERIV, u)
    return apply_odd(DERIV.T, [w[i] * grad[i] for i in range(5)])


def plane_terms(v0, v1, coef, hx, inv_hx, widths):
    n = len(widths)
    quarter, twelfth = hx * 0.25, hx * (1.0 / 12.0)
    cache = {}

    def weights(hy, hz):
        key = (round(hy, 12), round(hz, 12))
        if key not in cache:
            m = [[hy / 4 * hz / 4, hy / 4 * hz / 12], [hy / 12 * hz / 4, hy / 12 * hz / 12]]
            k = [
                [0.0, hy / 4 / hz],
                [hz / 4 / hy, hz / 12 / hy + hy / 12 / hz],
            ]
            cache[key] = (
                [[quarter * k[j][l] for l in range(2)] for j in range(2)],
                [[inv_hx * m[j][l] + twelfth * k[j][l] for l in range(2)] for j in range(2)],
            )
        return cache[key]

    near, far = {}, {}

    def add(store, key, value):
        store[key] = store[key] + value if key in store else value

    sums = {k: v0[k] + v1[k] for k in v0}
    diffs = {k: v0[k] - v1[k] for k in v0}
    back = [{}, {}]
    for b in range(n):
        line = {}
        for c in range(n):
            for xi, field in ((0, sums), (1, diffs)):
                lo, hi = (field[b, c], field[b + 1, c]), None
                ys = []
                for cc in (c, c + 1):
                    key = (xi, cc)
                    if key not in line:
                        line[key] = (
                            field[b, cc] + field[b + 1, cc],
                            field[b, cc] - field[b + 1, cc],
                        )
        zline = {}
        for c in range(n):
            ws, wd = weights(widths[b], widths[c])
            value = coef(b, c)
            for xi, w in ((0, ws), (1, wd)):
                for yi in range(2):
                    left, right = line[xi, c][yi], line[xi, c + 1][yi]
                    d = (w[yi][1] * value) * (left - right)
                    if xi == 0 and yi == 0:
                        add(zline, (xi, yi, c), d)
                        add(zline, (xi, yi, c + 1), -d)
                    else:
                        s = (w[yi][0] * value) * (left + right)
                        add(zline, (xi, yi, c), s + d)
                        add(zline, (xi, yi, c + 1), s - d)
        for c in range(n + 1):
            for xi in range(2):
                s, d = zline[xi, 0, c], zline[xi, 1, c]
                add(back[xi], (b, c), s + d)
                add(back[xi], (b + 1, c), s - d)
    for key in back[0]:
        near[key] = back[0][key] + back[1][key]
        far[key] = back[0][key] - back[1][key]
    return near, far


def replicated_kernel(
    ny, local, blocks_ref, solution_ref, residual_ref,
    weighted, expanded, out, coeff, winv, resid, guess, direction, iterate, picked,
):
    rows, lanes = weighted.shape[3:]
    halves = rows // 8

    def next_x(t):
        return pltpu.roll(t, rows - ny, 0)

    def next_y(t):
        return pltpu.roll(t, rows - 1, 0)

    def next_z(t):
        return pltpu.roll(t, lanes - 1, 1)

    def prev_x(t):
        return pltpu.roll(t, ny, 0)

    def prev_y(t):
        return pltpu.roll(t, 1, 0)

    def prev_z(t):
        return pltpu.roll(t, 1, 1)

    row = lax.broadcasted_iota(jnp.int32, (rows, lanes), 0)
    lane = lax.broadcasted_iota(jnp.int32, (rows, lanes), 1)
    keep_x = (row >= ny).astype(jnp.float32)
    keep_y = (lax.rem(row, ny) > 0).astype(jnp.float32)
    keep_z = (lane > 0).astype(jnp.float32)

    def masked(a, b, c, t):
        if a == 0:
            t = t * keep_x
        if b == 0:
            t = t * keep_y
        if c == 0:
            t = t * keep_z
        return t

    def phases(n):
        return [(a, b, c) for a in range(n) for b in range(n) for c in range(n)]

    def expand(n, get, put):
        for a in range(n):
            for b in range(n):
                put((a, b, n), next_z(get((a, b, 0))))
        for a in range(n):
            for c in range(n + 1):
                put((a, n, c), next_y(get((a, 0, c))))
        for b in range(n + 1):
            for c in range(n + 1):
                put((n, b, c), next_x(get((0, b, c))))

    def fold(n, get, put):
        for b in range(n + 1):
            for c in range(n + 1):
                put((0, b, c), get((0, b, c)) + prev_x(get((n, b, c))))
        for a in range(n):
            for c in range(n + 1):
                put((a, 0, c), get((a, 0, c)) + prev_y(get((a, n, c))))
        for a in range(n):
            for b in range(n):
                put((a, b, 0), get((a, b, 0)) + prev_z(get((a, b, n))))

    def put_in(ref):
        def put(k, t):
            ref[k] = t
        return put

    def get_from(ref):
        return lambda k: ref[k]

    first = lane < lanes // 2
    for a in range(5):
        for b in range(5):
            for c in range(5):
                w = float(QUAD[a] * QUAD[b] * QUAD[c])
                both = blocks_ref[:, (a * 5 + b) * 5 + c, :]
                lower, higher = both[:rows], both[rows:]
                kappa = jnp.where(first, lower, pltpu.roll(higher, lanes // 2, 1))
                source = jnp.where(first, pltpu.roll(lower, lanes // 2, 1), higher)
                expanded[a, b, c] = kappa
                weighted[a, b, c] = w * kappa
                out[a, b, c] = w * source
    fold(4, get_from(out), put_in(out))
    for k in phases(4):
        resid[k] = masked(*k, out[k])
        direction[k] = jnp.zeros((rows, lanes), jnp.float32)
        iterate[k] = jnp.zeros((rows, lanes), jnp.float32)

    for a in range(4):
        two = {
            (b, c): expanded[a, b, c] + expanded[a + 1, b, c]
            for b in range(5) for c in range(5)
        }
        two = {(b, c): two[b, c] + two[b + 1, c] for b in range(4) for c in range(5)}
        for b in range(4):
            for c in range(4):
                coeff[a, b, c] = 0.125 * (two[b, c] + two[b, c + 1])

    def halved(n, get):
        result = {}
        for a, b, c in phases(n // 2):
            t = None
            for x in range(2):
                for y in range(2):
                    for z in range(2):
                        v = get((2 * a + x, 2 * b + y, 2 * c + z))
                        t = v if t is None else t + v
            result[a, b, c] = 0.125 * t
        return result

    coeff1 = halved(4, get_from(coeff))
    coeff2 = halved(2, coeff1.__getitem__)

    def inverse_diagonal(n, widths, get, put):
        cells = {}
        for a, b, c in phases(n):
            x, y, z = widths[a], widths[b], widths[c]
            cells[a, b, c] = get((a, b, c)) * (
                y * z / (9.0 * x) + x * z / (9.0 * y) + x * y / (9.0 * z)
            )
        for axis, prev in ((0, prev_x), (1, prev_y), (2, prev_z)):
            sums = {}
            for k in phases(n):
                lower = list(k)
                lower[axis] = (k[axis] - 1) % n
                t = cells[tuple(lower)]
                sums[k] = cells[k] + (prev(t) if k[axis] == 0 else t)
            cells = sums
        for k in phases(n):
            put(k, masked(*k, relax_weight / cells[k]))

    inverse_diagonal(4, WIDTHS[0], get_from(coeff), put_in(winv))
    winv1, winv2 = {}, {}
    inverse_diagonal(2, WIDTHS[1], coeff1.__getitem__, winv1.__setitem__)
    inverse_diagonal(1, WIDTHS[2], coeff2.__getitem__, winv2.__setitem__)

    def lor_fine():
        expand(4, get_from(expanded), put_in(expanded))
        for b in range(5):
            for c in range(5):
                out[0, b, c] = jnp.zeros((rows, lanes), jnp.float32)

        def step(i, carry):
            a = lax.rem(i, 4)
            part = pl.ds(pl.multiple_of((i // 4) * 8, 8), 8)
            outer = (a == 0) | (a == 3)
            hx = jnp.where(outer, GAPS[0], GAPS[1])
            inv_hx = jnp.where(outer, 1.0 / GAPS[0], 1.0 / GAPS[1])
            keys = [(b, c) for b in range(5) for c in range(5)]
            v0 = {k: expanded[a, k[0], k[1], part, :] for k in keys}
            v1 = {k: expanded[a + 1, k[0], k[1], part, :] for k in keys}
            near, far = plane_terms(
                v0, v1, lambda b, c: coeff[a, b, c, part, :], hx, inv_hx, GAPS
            )
            for b, c in keys:
                out[a, b, c, part, :] += near[b, c]
                out[a + 1, b, c, part, :] = far[b, c]
            return carry

        lax.fori_loop(0, 4 * halves, step, 0)
        fold(4, get_from(out), put_in(out))

    def lor_coarse(field, n, widths, coefs):
        v = dict(field)
        expand(n, v.__getitem__, v.__setitem__)
        total = {}
        for a in range(n):
            keys = [(b, c) for b in range(n + 1) for c in range(n + 1)]
            near, far = plane_terms(
                {k: v[(a,) + k] for k in keys},
                {k: v[(a + 1,) + k] for k in keys},
                lambda b, c: coefs[a, b, c],
                widths[a],
                1.0 / widths[a],
                widths,
            )
            for k in keys:
                key = (a,) + k
                total[key] = total[key] + near[k] if key in total else near[k]
                total[(a + 1,) + k] = far[k]
        fold(n, total.__getitem__, total.__setitem__)
        return total

    def shares(widths):
        left, right = [], []
        for i in range(len(widths) // 2):
            span = widths[2 * i] + widths[2 * i + 1]
            left.append(widths[2 * i + 1] / span)
            right.append(widths[2 * i] / span)
        return left, right

    def restrict_phases(field, n, widths):
        left, right = shares(widths)
        half = n // 2
        sizes = [n, n, n]
        for axis, prev in ((2, prev_z), (1, prev_y), (0, prev_x)):
            sizes[axis] = half
            coarse = {}
            for a in range(sizes[0]):
                for b in range(sizes[1]):
                    for c in range(sizes[2]):
                        k = (a, b, c)
                        j = k[axis]

                        def at(i):
                            return field[k[:axis] + (i,) + k[axis + 1:]]

                        if j == 0:
                            before = right[half - 1] * prev(at(n - 1))
                        else:
                            before = right[j - 1] * at(2 * j - 1)
                        coarse[k] = at(2 * j) + left[j] * at(2 * j + 1) + before
            field = coarse
        return field

    def prolong_phases(field, n, widths):
        left, right = shares(widths)
        half = n // 2
        sizes = [half, half, half]
        for axis, following in ((0, next_x), (1, next_y), (2, next_z)):
            sizes[axis] = n
            fine = {}
            for a in range(sizes[0]):
                for b in range(sizes[1]):
                    for c in range(sizes[2]):
                        k = (a, b, c)
                        i, odd = divmod(k[axis], 2)

                        def at(j):
                            return field[k[:axis] + (j,) + k[axis + 1:]]

                        if odd:
                            after = following(at(0)) if i + 1 == half else at(i + 1)
                            fine[k] = left[i] * at(i) + right[i] * after
                        else:
                            fine[k] = at(i)
            field = fine
        return field

    def precondition():
        for k in phases(4):
            t = winv[k] * resid[k]
            guess[k] = t
            expanded[k] = t
        lor_fine()
        defect = {k: resid[k] - out[k] for k in phases(4)}
        f1 = restrict_phases(defect, 4, WIDTHS[0])
        g1 = {k: winv1[k] * f1[k] for k in f1}
        l1 = lor_coarse(g1, 2, WIDTHS[1], coeff1)
        f2 = restrict_phases({k: f1[k] - l1[k] for k in f1}, 2, WIDTHS[1])
        g2 = {k: winv2[k] * f2[k] for k in f2}
        l2 = lor_coarse(g2, 1, WIDTHS[2], coeff2)
        g2 = {k: g2[k] + winv2[k] * (f2[k] - l2[k]) for k in f2}
        p1 = prolong_phases(g2, 2, WIDTHS[1])
        g1 = {k: g1[k] + p1[k] for k in f1}
        l1 = lor_coarse(g1, 2, WIDTHS[1], coeff1)
        g1 = {k: g1[k] + winv1[k] * (f1[k] - l1[k]) for k in f1}
        p0 = prolong_phases(g1, 4, WIDTHS[0])
        for k in phases(4):
            t = guess[k] + p0[k]
            guess[k] = t
            expanded[k] = t
        lor_fine()

    def operator():
        expand(4, get_from(expanded), put_in(expanded))

        def plane(i, carry):
            a = lax.rem(i, 5)
            part = pl.ds(pl.multiple_of((i // 5) * 8, 8), 8)
            total = {}
            u = {(b, c): expanded[a, b, c, part, :] for b in range(5) for c in range(5)}
            w = {(b, c): weighted[a, b, c, part, :] for b in range(5) for c in range(5)}
            for c in range(5):
                y = line_terms([u[b, c] for b in range(5)], [w[b, c] for b in range(5)])
                for b in range(5):
                    total[b, c] = y[b]
            for b in range(5):
                y = line_terms([u[b, c] for c in range(5)], [w[b, c] for c in range(5)])
                for c in range(5):
                    out[a, b, c, part, :] = total[b, c] + y[c]
            return carry

        lax.fori_loop(0, 5 * halves, plane, 0)

        def columns(i, carry):
            b = lax.rem(i, 5)
            part = pl.ds(pl.multiple_of((i // 5) * 8, 8), 8)
            for c in range(5):
                y = line_terms(
                    [expanded[a, b, c, part, :] for a in range(5)],
                    [weighted[a, b, c, part, :] for a in range(5)],
                )
                for a in range(5):
                    out[a, b, c, part, :] += y[a]
            return carry

        lax.fori_loop(0, 5 * halves, columns, 0)
        fold(4, get_from(out), put_in(out))

    def iteration(_, rho_old):
        precondition()
        total = jnp.zeros((rows, lanes), jnp.float32)
        for k in phases(4):
            r = resid[k]
            z = guess[k] + winv[k] * (r - out[k])
            guess[k] = z
            total = total + r * z
        rho = jnp.sum(total, axis=(0, 1), keepdims=True)
        beta = rho / rho_old
        for k in phases(4):
            p = guess[k] + beta * direction[k]
            direction[k] = p
            expanded[k] = p
        operator()
        total = jnp.zeros((rows, lanes), jnp.float32)
        for k in phases(4):
            total = total + direction[k] * out[k]
        alpha = rho / jnp.sum(total, axis=(0, 1), keepdims=True)
        for k in phases(4):
            iterate[k] += alpha * direction[k]
            resid[k] -= masked(*k, alpha * out[k])
        return rho

    lax.fori_loop(0, 2, iteration, jnp.ones((1, 1), jnp.float32))

    base = lax.axis_index("gx") * ny + lax.axis_index("gy")
    start = lax.axis_index("gz") * local
    for index, field in enumerate((iterate, resid)):
        for a in range(1, 5):
            for b in range(1, 5):
                at = lax.rem(base + (a // 4) * ny + b // 4, rows)
                for c in range(4):
                    picked[c, pl.ds(16 * index + 4 * (a - 1) + b - 1, 1), :] = field[
                        a % 4, b % 4, c, pl.ds(at, 1), :
                    ]
    width = solution_ref.shape[2]
    lane_in = lax.broadcasted_iota(jnp.int32, (lanes, width), 0)
    lane_out = lax.broadcasted_iota(jnp.int32, (lanes, width), 1)
    total = jnp.zeros((32, width), jnp.float32)
    for slot in range(4):
        t = picked[1 + slot] if slot < 3 else next_z(picked[0])
        hot = (lane_out == 4 * (lane_in - start) + slot).astype(jnp.bfloat16)
        high = t.astype(jnp.bfloat16)
        rest = t - high.astype(jnp.float32)
        middle = rest.astype(jnp.bfloat16)
        low = (rest - middle.astype(jnp.float32)).astype(jnp.bfloat16)
        parts = jnp.dot(
            jnp.concatenate([high, middle, low], axis=0), hot,
            preferred_element_type=jnp.float32,
        )
        total = total + ((parts[:32] + parts[32:64]) + parts[64:])
    for i in range(4):
        solution_ref[i] = total[4 * i : 4 * i + 4]
        residual_ref[i] = total[16 + 4 * i : 20 + 4 * i]


def flipped(index, bits):
    step = 1
    while step <= bits:
        if bits & step:
            index = index + step - 2 * step * lax.rem(index // step, 2)
        step *= 2
    return index


def gather_kernel(block_ref, all_ref, own_sem, send_sem, recv_sem):
    gx, gy, gz = (lax.axis_index(name) for name in ("gx", "gy", "gz"))
    nx, ny = lax.axis_size("gx"), lax.axis_size("gy")
    rows = block_ref.shape[0]
    upper = rows // 16 * 8
    mesh_id = pl.DeviceIdType.MESH
    cross_x = lax.rem(gx + 2, nx)
    twin = gx + 1 - 2 * lax.rem(gx, 2)
    cross_z = 1 - gz
    to_x, to_z, to_twin = (cross_x, gy, gz), (gx, gy, cross_z), (twin, gy, gz)
    ys = [flipped(gy, d) for d in range(ny)]
    to_y = [(gx, y, gz) for y in ys[1:]]

    barrier = pltpu.get_barrier_semaphore()
    peers = to_y + [to_x, to_z, to_twin]
    for peer in peers:
        pl.semaphore_signal(barrier, inc=1, device_id=peer, device_id_type=mesh_id)
    pl.semaphore_wait(barrier, len(peers))

    def slot(z, x, y):
        return (z * nx + x) * ny + y

    started = []

    def send(src, dst, device):
        number = len(started)
        copy = pltpu.make_async_remote_copy(
            src_ref=src,
            dst_ref=dst,
            send_sem=send_sem.at[number],
            recv_sem=recv_sem.at[number],
            device_id=device,
            device_id_type=mesh_id,
        )
        copy.start()
        started.append(copy)
        return copy

    mine = all_ref.at[slot(gz, gx, gy)]
    along = [None] + [send(block_ref, mine, device) for device in to_y]
    own = pltpu.make_async_copy(block_ref, mine, own_sem)
    own.start()
    by_x, by_z, by_xz, by_zx, last = {}, {}, {}, {}, []

    def column(d):
        if d:
            along[d].wait_recv()
        here = all_ref.at[slot(gz, gx, ys[d])]
        src = here if d else block_ref
        by_x[d] = send(src, here, to_x)
        by_z[d] = send(src, here, to_z)
        last.append(send(src, here, to_twin))

    def onward(d):
        by_x[d].wait_recv()
        number = slot(gz, cross_x, ys[d])
        part = all_ref.at[number, pl.ds(0, upper)]
        by_xz[d] = send(part, part, to_z)
        last.append(send(all_ref.at[number], all_ref.at[number], to_twin))
        by_z[d].wait_recv()
        number = slot(cross_z, gx, ys[d])
        part = all_ref.at[number, pl.ds(upper, rows - upper)]
        by_zx[d] = send(part, part, to_x)
        last.append(send(all_ref.at[number], all_ref.at[number], to_twin))

    column(0)
    for d in range(1, ny):
        column(d)
        onward(d - 1)
    onward(ny - 1)
    for d in range(ny):
        by_xz[d].wait_recv()
        by_zx[d].wait_recv()
        here = all_ref.at[slot(cross_z, cross_x, ys[d])]
        last.append(send(here, here, to_twin))
    for copy in last:
        copy.wait_recv()
    own.wait()
    for copy in started:
        copy.wait_send()


def replicated_body(kappa, source):
    local = kappa.shape[5]
    nx, ny, nz = (lax.axis_size(name) for name in ("gx", "gy", "gz"))
    vmem = pl.BlockSpec(memory_space=pltpu.VMEM)
    block = jnp.concatenate([kappa, source], axis=5).reshape(125, 2 * local)
    copies = (ny - 1) + 8 * ny
    blocks = pl.pallas_call(
        gather_kernel,
        out_shape=pltpu.VMEM((nz * nx * ny,) + block.shape, jnp.float32),
        in_specs=[vmem],
        out_specs=vmem,
        scratch_shapes=[
            pltpu.SemaphoreType.DMA,
            pltpu.SemaphoreType.DMA((copies,)),
            pltpu.SemaphoreType.DMA((copies,)),
        ],
        compiler_params=pltpu.CompilerParams(collective_id=0, has_side_effects=True),
        name="gather",
    )(block)
    rows, lanes = nx * ny, nz * local

    def field(n):
        return pltpu.VMEM((n, n, n, rows, lanes), jnp.float32)

    outs = pl.pallas_call(
        lambda *refs: replicated_kernel(ny, local, *refs),
        out_shape=[jax.ShapeDtypeStruct((4, 4, 4 * local), jnp.float32)] * 2,
        in_specs=[vmem],
        out_specs=[vmem, vmem],
        scratch_shapes=[field(5), field(5), field(5)] + [field(4)] * 6
        + [pltpu.VMEM((4, 32, lanes), jnp.float32)],
        name="replicated",
    )(pltpu.with_memory_space_constraint(blocks, pltpu.VMEM))

    return outs[0], outs[1]


def body(kappa, source):
    nx, ny, nz = (lax.axis_size(name) for name in ("gx", "gy", "gz"))
    local_x, local_y, local_z = kappa.shape[3:]
    rows, lanes = nx * ny, nz * local_z
    small = rows % 8 == 0 and lanes == 128 and rows <= 64
    if local_x == 1 and local_y == 1 and nx == 4 and nz == 2 and ny & (ny - 1) == 0 and small:
        return replicated_body(kappa, source)
    return distributed_body(kappa, source)


def solution(mesh):
    placed = (P(None, None, None, "gx", "gy", "gz"), P(None, None, None, "gx", "gy", "gz"))
    return jax.shard_map(
        body,
        mesh=mesh,
        in_specs=placed,
        out_specs=(P("gx", "gy", "gz"), P("gx", "gy", "gz")),
        check_vma=False,
    )
```
